16 devices in a mesh: dp: 2 (over z), sp: 8 (over y, x, core).
Axes of the slice: x: 2, y: 2, z: 2, core: 2. Of those that a mesh axis runs over, the one named last changes fastest.
Arguments:
- hidden: bfloat16 [6144, 3072], P(('dp', 'sp')), parts along dimension 0
- grad_out: bfloat16 [6144, 3072], P(('dp', 'sp')), parts along dimension 0
- positions: int32 [6144], P(('dp', 'sp')), parts along dimension 0
- doc_ids: int32 [6144], P(('dp', 'sp')), parts along dimension 0
- w_q: bfloat16 [3072, 3072], replicated
- w_k: bfloat16 [3072, 1024], replicated
- w_v: bfloat16 [3072, 1024], replicated
- w_o: bfloat16 [3072, 3072], replicated
Outputs:
- output 1: bfloat16 [6144, 3072], P(('dp', 'sp')), parts along dimension 0
- output 2: bfloat16 [6144, 3072], P(('dp', 'sp')), parts along dimension 0
- output 3: float32 [6144, 3072], P('dp'), parts along dimension 0
- output 4: float32 [6144, 1024], P('dp'), parts along dimension 0
- output 5: float32 [6144, 1024], P('dp'), parts along dimension 0
- output 6: float32 [6144, 3072], P('dp'), parts along dimension 0
There are 2 independent parts. The reference program is written for one: setup_inputs(seed, part) draws one part's arguments, and reference() takes and returns one part's arrays. A program takes and returns all parts, laid end to end along the dimension named above; an argument that names none is the same for every part.
All inputs are finite; a program needn't handle non-finite values.
Results may differ from the reference program's by a relative error of at most 0.0106679.
Values are sent between devices in bfloat16 or wider.
A program may use at most 1 GiB of HBM per device.

```python
import jax
import jax.numpy as jnp
from jax import lax

D = 3072
HEADS = 24
KV_HEADS = 8
HEAD = 128
SEQ = 3072

ROPE_THETA = 500000.0
ROPE_FACTOR = 8.0
ROPE_LOW = 1.0
ROPE_HIGH = 4.0
ROPE_OLD_CTX = 8192.0
SCORE_LIMIT = 32 * 1024 * 1024
NEG_BIG = -1.0e30


def draw_layout(layout_key):
    cut_key, start_key = jax.random.split(layout_key)
    cut_points = jnp.sort(jax.random.randint(cut_key, (2,), SEQ // 8, SEQ - SEQ // 8))
    token_idx = jnp.arange(SEQ, dtype=jnp.int32)
    doc_ids = jnp.sum(token_idx[:, None] >= cut_points[None, :], axis=1).astype(jnp.int32)
    bounds = jnp.concatenate([jnp.zeros((1,), jnp.int32), cut_points.astype(jnp.int32)])
    starts = jax.random.randint(start_key, (3,), 0, SEQ)
    positions = (starts[doc_ids] + token_idx - bounds[doc_ids]).astype(jnp.int32)
    return positions, doc_ids


def setup_inputs(seed: int = 0, part: int = 0) -> dict:
    part_key = jax.random.fold_in(jax.random.key(seed), part)
    hid_key, grad_key, layout_key = jax.random.split(part_key, 3)
    weight_keys = jax.random.split(jax.random.key(seed + 1), 4)
    hidden = jax.random.normal(hid_key, (SEQ, D), jnp.float32).astype(jnp.bfloat16)
    grad_out = jax.random.normal(grad_key, (SEQ, D), jnp.float32).astype(jnp.bfloat16)
    positions, doc_ids = draw_layout(layout_key)
    in_scale = D ** -0.5
    w_q = (jax.random.normal(weight_keys[0], (D, HEADS * HEAD), jnp.float32) * in_scale).astype(jnp.bfloat16)
    w_k = (jax.random.normal(weight_keys[1], (D, KV_HEADS * HEAD), jnp.float32) * in_scale).astype(jnp.bfloat16)
    w_v = (jax.random.normal(weight_keys[2], (D, KV_HEADS * HEAD), jnp.float32) * in_scale).astype(jnp.bfloat16)
    w_o = (jax.random.normal(weight_keys[3], (HEADS * HEAD, D), jnp.float32) * (HEADS * HEAD) ** -0.5).astype(jnp.bfloat16)
    return {"hidden": hidden, "grad_out": grad_out, "positions": positions, "doc_ids": doc_ids, "w_q": w_q, "w_k": w_k, "w_v": w_v, "w_o": w_o}


def rope_freqs():
    half_idx = jnp.arange(HEAD // 2, dtype=jnp.float32)
    inv_freq = jnp.power(ROPE_THETA, -2.0 * half_idx / HEAD)
    wavelen = 2.0 * jnp.pi / inv_freq
    smooth = (ROPE_OLD_CTX / wavelen - ROPE_LOW) / (ROPE_HIGH - ROPE_LOW)
    mixed_freq = (1.0 - smooth) * inv_freq / ROPE_FACTOR + smooth * inv_freq
    scaled = jnp.where(wavelen > ROPE_OLD_CTX / ROPE_LOW, inv_freq / ROPE_FACTOR, mixed_freq)
    return jnp.where(wavelen < ROPE_OLD_CTX / ROPE_HIGH, inv_freq, scaled)


def rope_tables(pos_vec):
    angles = pos_vec.astype(jnp.float32)[:, None] * rope_freqs()[None, :]
    return jnp.cos(angles)[:, None, :], jnp.sin(angles)[:, None, :]


def rotate(values, cos_tab, sin_tab):
    half_dim = values.shape[-1] // 2
    first_half = values[..., :half_dim]
    second_half = values[..., half_dim:]
    return jnp.concatenate([first_half * cos_tab - second_half * sin_tab, second_half * cos_tab + first_half * sin_tab], axis=-1)


def block_rows(n_query, head_count, n_keys):
    block_len = n_query
    while block_len % 16 == 0 and head_count * block_len * n_keys > SCORE_LIMIT:
        block_len = block_len // 2
    return block_len


def block_probs(q_blk, k_all, pos_blk, doc_blk, pos_all, doc_all):
    scores = jnp.einsum("qhgd,shd->hgqs", q_blk, k_all) * HEAD ** -0.5
    allowed = (pos_all[None, :] <= pos_blk[:, None]) & (doc_all[None, :] == doc_blk[:, None])
    scores = jnp.where(allowed, scores, NEG_BIG)
    row_peak = jnp.max(scores, axis=-1, keepdims=True)
    exp_vals = jnp.exp(scores - row_peak)
    return exp_vals / jnp.sum(exp_vals, axis=-1, keepdims=True)


def reference(hidden, grad_out, positions, doc_ids, w_q, w_k, w_v, w_o):
    group_size = HEADS // KV_HEADS
    score_scale = HEAD ** -0.5
    cos_tab, sin_tab = rope_tables(positions)
    q_pre = jnp.dot(hidden, w_q, preferred_element_type=jnp.float32).reshape(SEQ, HEADS, HEAD)
    k_pre = jnp.dot(hidden, w_k, preferred_element_type=jnp.float32).reshape(SEQ, KV_HEADS, HEAD)
    v_pre = jnp.dot(hidden, w_v, preferred_element_type=jnp.float32).reshape(SEQ, KV_HEADS, HEAD)
    q_rot = rotate(q_pre, cos_tab, sin_tab).astype(jnp.bfloat16).astype(jnp.float32)
    k_rot = rotate(k_pre, cos_tab, sin_tab).astype(jnp.bfloat16).astype(jnp.float32)
    v_val = v_pre.astype(jnp.bfloat16).astype(jnp.float32)
    block_len = block_rows(SEQ, HEADS, SEQ)
    n_blocks = SEQ // block_len
    q_blocks = q_rot.reshape(n_blocks, block_len, KV_HEADS, group_size, HEAD)
    pos_blocks = positions.reshape(n_blocks, block_len)
    doc_blocks = doc_ids.reshape(n_blocks, block_len)

    def fwd_block(block_in):
        q_blk, pos_blk, doc_blk = block_in
        prob_f32 = block_probs(q_blk, k_rot, pos_blk, doc_blk, positions, doc_ids)
        prob_bf = prob_f32.astype(jnp.bfloat16).astype(jnp.float32)
        return jnp.einsum("hgqs,shd->qhgd", prob_bf, v_val).astype(jnp.bfloat16)

    context = lax.map(fwd_block, (q_blocks, pos_blocks, doc_blocks)).reshape(SEQ, HEADS * HEAD)
    attn_out = jnp.dot(context, w_o, preferred_element_type=jnp.float32).astype(jnp.bfloat16)

    d_ctx = jnp.dot(grad_out, w_o.T, preferred_element_type=jnp.float32).astype(jnp.bfloat16)
    grad_wo = jnp.dot(context.T, grad_out, preferred_element_type=jnp.float32)
    d_ctx_blocks = d_ctx.astype(jnp.float32).reshape(n_blocks, block_len, KV_HEADS, group_size, HEAD)

    def bwd_block(acc_pair, block_in):
        dk_acc, dv_acc = acc_pair
        q_blk, dctx_blk, pos_blk, doc_blk = block_in
        prob_f32 = block_probs(q_blk, k_rot, pos_blk, doc_blk, positions, doc_ids)
        prob_bf = prob_f32.astype(jnp.bfloat16).astype(jnp.float32)
        d_prob = jnp.einsum("qhgd,shd->hgqs", dctx_blk, v_val)
        row_dot = jnp.sum(prob_f32 * d_prob, axis=-1, keepdims=True)
        d_score = (prob_f32 * (d_prob - row_dot) * score_scale).astype(jnp.bfloat16).astype(jnp.float32)
        dq_blk = jnp.einsum("hgqs,shd->qhgd", d_score, k_rot).astype(jnp.bfloat16)
        dk_acc = dk_acc + jnp.einsum("hgqs,qhgd->shd", d_score, q_blk)
        dv_acc = dv_acc + jnp.einsum("hgqs,qhgd->shd", prob_bf, dctx_blk)
        return (dk_acc, dv_acc), dq_blk

    zero_acc = jnp.zeros((SEQ, KV_HEADS, HEAD), jnp.float32)
    (dk_acc, dv_acc), dq_blocks = lax.scan(bwd_block, (zero_acc, zero_acc), (q_blocks, d_ctx_blocks, pos_blocks, doc_blocks))
    dq_rot = dq_blocks.reshape(SEQ, HEADS, HEAD).astype(jnp.float32)
    dq_pre = rotate(dq_rot, cos_tab, -sin_tab).astype(jnp.bfloat16).reshape(SEQ, HEADS * HEAD)
    dk_rot = dk_acc.astype(jnp.bfloat16).astype(jnp.float32)
    dk_pre = rotate(dk_rot, cos_tab, -sin_tab).astype(jnp.bfloat16).reshape(SEQ, KV_HEADS * HEAD)
    dv_pre = dv_acc.astype(jnp.bfloat16).reshape(SEQ, KV_HEADS * HEAD)
    grad_hidden = (jnp.dot(dq_pre, w_q.T, preferred_element_type=jnp.float32) + jnp.dot(dk_pre, w_k.T, preferred_element_type=jnp.float32) + jnp.dot(dv_pre, w_v.T, preferred_element_type=jnp.float32)).astype(jnp.bfloat16)
    grad_wq = jnp.dot(hidden.T, dq_pre, preferred_element_type=jnp.float32)
    grad_wk = jnp.dot(hidden.T, dk_pre, preferred_element_type=jnp.float32)
    grad_wv = jnp.dot(hidden.T, dv_pre, preferred_element_type=jnp.float32)
    return attn_out, grad_hidden, grad_wq, grad_wk, grad_wv, grad_wo
```

```python
import functools
import math

import jax
import jax.numpy as jnp
from jax import lax
from jax.experimental import pallas as pl
from jax.experimental.pallas import tpu as pltpu
from jax.sharding import PartitionSpec as P


HEAD_DIM = 128
HALF = HEAD_DIM // 2
ROPE_THETA = 500000.0
ROPE_FACTOR = 8.0
ROPE_LOW = 1.0
ROPE_HIGH = 4.0
ROPE_OLD_CTX = 8192.0
NEG_BIG = -1.0e30
BLK = 256
F32 = jnp.float32
BF16 = jnp.bfloat16


def rope_freqs():
    half_idx = jnp.arange(HALF, dtype=F32)
    inv_freq = jnp.power(ROPE_THETA, -2.0 * half_idx / HEAD_DIM)
    wavelen = 2.0 * jnp.pi / inv_freq
    smooth = (ROPE_OLD_CTX / wavelen - ROPE_LOW) / (ROPE_HIGH - ROPE_LOW)
    mixed_freq = (1.0 - smooth) * inv_freq / ROPE_FACTOR + smooth * inv_freq
    scaled = jnp.where(wavelen > ROPE_OLD_CTX / ROPE_LOW, inv_freq / ROPE_FACTOR, mixed_freq)
    return jnp.where(wavelen < ROPE_OLD_CTX / ROPE_HIGH, inv_freq, scaled)


def dot_nn(lhs, rhs):
    return lax.dot_general(lhs, rhs, (((1,), (0,)), ((), ())), preferred_element_type=F32)


def dot_nt(lhs, rhs):
    return lax.dot_general(lhs, rhs, (((1,), (1,)), ((), ())), preferred_element_type=F32)


def dot_tn(lhs, rhs):
    return lax.dot_general(lhs, rhs, (((0,), (0,)), ((), ())), preferred_element_type=F32)


def dot_tt(lhs, rhs):
    return lax.dot_general(lhs, rhs, (((0,), (1,)), ((), ())), preferred_element_type=F32)


def proj_kernel(group, x_ref, g_ref, wq_ref, wk_ref, wv_ref, wo_ref, cos_ref, sin_ref, out_ref):
    cos_tab, sin_tab = cos_ref[...], sin_ref[...]

    def rope(val):
        return (val * cos_tab + pltpu.roll(val, HALF, 1) * sin_tab).astype(BF16)

    width = group * HEAD_DIM
    q_val = dot_nn(x_ref[...], wq_ref[...])
    for head in range(group):
        cols = slice(head * HEAD_DIM, (head + 1) * HEAD_DIM)
        out_ref[0, :, cols] = rope(q_val[:, cols])
    out_ref[0, :, width:2 * width] = dot_nt(g_ref[...], wo_ref[...]).astype(BF16)
    out_ref[0, :, 2 * width:2 * width + HEAD_DIM] = rope(dot_nn(x_ref[...], wk_ref[...]))
    out_ref[0, :, 2 * width + HEAD_DIM:] = dot_nn(x_ref[...], wv_ref[...]).astype(BF16)


def project(hidden, grad_out, w_q, w_k, w_v, w_o, cos_tab, sin_tab, n_dev, group):
    tokens, width = hidden.shape
    cols = group * HEAD_DIM
    total = 2 * cols + 2 * HEAD_DIM
    flops = 2 * tokens * width * n_dev * total
    return pl.pallas_call(
        functools.partial(proj_kernel, group),
        grid=(n_dev,),
        in_specs=[
            pl.BlockSpec((tokens, width), lambda i: (0, 0)),
            pl.BlockSpec((tokens, width), lambda i: (0, 0)),
            pl.BlockSpec((width, cols), lambda i: (0, i)),
            pl.BlockSpec((width, HEAD_DIM), lambda i: (0, i)),
            pl.BlockSpec((width, HEAD_DIM), lambda i: (0, i)),
            pl.BlockSpec((cols, width), lambda i: (i, 0)),
            pl.BlockSpec((tokens, HEAD_DIM), lambda i: (0, 0)),
            pl.BlockSpec((tokens, HEAD_DIM), lambda i: (0, 0)),
        ],
        out_specs=pl.BlockSpec((1, tokens, total), lambda i: (i, 0, 0)),
        out_shape=jax.ShapeDtypeStruct((n_dev, tokens, total), BF16),
        compiler_params=pltpu.CompilerParams(dimension_semantics=("arbitrary",), vmem_limit_bytes=48 * 1024 * 1024),
        cost_estimate=pl.CostEstimate(flops=flops, bytes_accessed=60_000_000, transcendentals=0),
        name="project",
    )(hidden, grad_out, w_q, w_k, w_v, w_o, cos_tab, sin_tab)


def attn_kernel(group, lo_ref, q_ref, do_ref, k_ref, v_ref, start_ref, cos_ref, sin_ref,
                ctx_lo, ctx_hi, dq_lo, dq_hi, dk_ref, dv_ref,
                s_scr, dp_scr, dk_acc, dv_acc, kt_scr, vt_scr, ctx_acc, dq_acc):
    blk = pl.program_id(0)
    n_blk = pl.num_programs(0)
    seq = k_ref.shape[0]
    scale = HEAD_DIM ** -0.5
    exp_scale = scale * math.log2(math.e)

    @pl.when(blk == 0)
    def _():
        dk_acc[...] = jnp.zeros_like(dk_acc)
        dv_acc[...] = jnp.zeros_like(dv_acc)

        @pl.loop(0, seq // BLK)
        def _(c):
            rows = pl.ds(pl.multiple_of(c * BLK, BLK), BLK)
            kt_scr[:, rows] = k_ref[rows, :].astype(F32).T.astype(BF16)
            vt_scr[:, rows] = v_ref[rows, :].astype(F32).T.astype(BF16)

    first = lo_ref[blk]
    last = blk + 1
    heads = [slice(h * HEAD_DIM, (h + 1) * HEAD_DIM) for h in range(group)]
    lanes = [slice(h * BLK, (h + 1) * BLK) for h in range(group)]
    starts = start_ref[...]
    q_idx = blk * BLK + lax.broadcasted_iota(jnp.int32, (1, BLK), 1)
    key_iota = lax.broadcasted_iota(jnp.int32, (BLK, BLK), 0)

    def score_step(c, peaks):
        rows = pl.ds(pl.multiple_of(c * BLK, BLK), BLK)
        key_idx = key_iota + c * BLK
        allowed = (key_idx >= starts) & (key_idx <= q_idx)
        k_blk = k_ref[rows, :]
        out = []
        for h in range(group):
            scores = jnp.where(allowed, dot_nt(k_blk, q_ref[:, heads[h]]), NEG_BIG)
            s_scr[rows, lanes[h]] = scores
            out.append(jnp.maximum(peaks[h], jnp.max(scores, axis=0, keepdims=True)))
        return tuple(out)

    peaks = lax.fori_loop(first, last, score_step, tuple(jnp.full((1, BLK), NEG_BIG, F32) for _ in range(group)))
    peaks = tuple(peak * exp_scale for peak in peaks)

    def exp_step(c, sums):
        rows = pl.ds(pl.multiple_of(c * BLK, BLK), BLK)
        v_blk = v_ref[rows, :]
        out = []
        for h in range(group):
            probs = jnp.exp2(s_scr[rows, lanes[h]] * exp_scale - peaks[h])
            d_prob = dot_nt(v_blk, do_ref[:, heads[h]])
            s_scr[rows, lanes[h]] = probs
            dp_scr[rows, lanes[h]] = d_prob
            out.append(sums[2 * h] + jnp.sum(probs, axis=0, keepdims=True))
            out.append(sums[2 * h + 1] + jnp.sum(probs * d_prob, axis=0, keepdims=True))
        return tuple(out)

    sums = lax.fori_loop(first, last, exp_step, tuple(jnp.zeros((1, BLK), F32) for _ in range(2 * group)))
    inv_sum = [1.0 / sums[2 * h] for h in range(group)]
    row_dot = [sums[2 * h + 1] * inv_sum[h] for h in range(group)]

    ctx_acc[...] = jnp.zeros_like(ctx_acc)
    dq_acc[...] = jnp.zeros_like(dq_acc)

    def grad_step(c, carry):
        rows = pl.ds(pl.multiple_of(c * BLK, BLK), BLK)
        k_t, v_t = kt_scr[:, rows], vt_scr[:, rows]
        dk_sum, dv_sum = dk_acc[rows, :], dv_acc[rows, :]
        for h in range(group):
            probs = s_scr[rows, lanes[h]] * inv_sum[h]
            probs_bf = probs.astype(BF16)
            d_score = (probs * (dp_scr[rows, lanes[h]] - row_dot[h]) * scale).astype(BF16)
            ctx_acc[:, lanes[h]] += dot_nn(v_t, probs_bf)
            dq_acc[:, lanes[h]] += dot_nn(k_t, d_score)
            dk_sum = dk_sum + dot_nn(d_score, q_ref[:, heads[h]])
            dv_sum = dv_sum + dot_nn(probs_bf, do_ref[:, heads[h]])
        dk_acc[rows, :] = dk_sum
        dv_acc[rows, :] = dv_sum
        return carry

    lax.fori_loop(first, last, grad_step, 0)

    def unrope(val, cos_tab, sin_tab):
        upper, lower = val[:HALF], val[HALF:]
        return (upper * cos_tab + lower * sin_tab).astype(BF16), (lower * cos_tab - upper * sin_tab).astype(BF16)

    own = pl.ds(pl.multiple_of(blk * BLK, BLK), BLK)
    cos_q, sin_q = cos_ref[:, own], sin_ref[:, own]
    half = ctx_lo.shape[0]
    for h in range(group):
        ctx_val = ctx_acc[:, lanes[h]].astype(BF16)
        dq_val = unrope(dq_acc[:, lanes[h]].astype(BF16).astype(F32), cos_q, sin_q)
        for part in range(2):
            row = h * HEAD_DIM + part * HALF
            ctx_out, dq_out = (ctx_lo, dq_lo) if row < half else (ctx_hi, dq_hi)
            place = slice(row % half, row % half + HALF)
            ctx_out[place, :] = ctx_val[part * HALF:(part + 1) * HALF]
            dq_out[place, :] = dq_val[part]

    @pl.when(blk == n_blk - 1)
    def _():
        @pl.loop(0, seq // BLK)
        def _(c):
            rows = pl.ds(pl.multiple_of(c * BLK, BLK), BLK)
            upper, lower = unrope(dk_acc[rows, :].T.astype(BF16).astype(F32), cos_ref[:, rows], sin_ref[:, rows])
            dk_ref[:HALF, rows] = upper
            dk_ref[HALF:, rows] = lower
            dv_ref[:, rows] = dv_acc[rows, :].T.astype(BF16)


def attention(packed, first_blk, starts, cos_t, sin_t, group):
    seq = packed.shape[0]
    cols = group * HEAD_DIM
    n_blk = seq // BLK
    grid_spec = pltpu.PrefetchScalarGridSpec(
        num_scalar_prefetch=1,
        grid=(n_blk,),
        in_specs=[
            pl.BlockSpec((BLK, cols), lambda i, lo: (i, 0)),
            pl.BlockSpec((BLK, cols), lambda i, lo: (i, 1)),
            pl.BlockSpec((seq, HEAD_DIM), lambda i, lo: (0, 2 * group)),
            pl.BlockSpec((seq, HEAD_DIM), lambda i, lo: (0, 2 * group + 1)),
            pl.BlockSpec((1, BLK), lambda i, lo: (0, i)),
            pl.BlockSpec((HALF, seq), lambda i, lo: (0, 0)),
            pl.BlockSpec((HALF, seq), lambda i, lo: (0, 0)),
        ],
        out_specs=[
            pl.BlockSpec((cols // 2, BLK), lambda i, lo: (0, i)),
            pl.BlockSpec((cols // 2, BLK), lambda i, lo: (0, i)),
            pl.BlockSpec((cols // 2, BLK), lambda i, lo: (0, i)),
            pl.BlockSpec((cols // 2, BLK), lambda i, lo: (0, i)),
            pl.BlockSpec((HEAD_DIM, seq), lambda i, lo: (0, 0)),
            pl.BlockSpec((HEAD_DIM, seq), lambda i, lo: (0, 0)),
        ],
        scratch_shapes=[
            pltpu.VMEM((seq, group * BLK), F32),
            pltpu.VMEM((seq, group * BLK), F32),
            pltpu.VMEM((seq, HEAD_DIM), F32),
            pltpu.VMEM((seq, HEAD_DIM), F32),
            pltpu.VMEM((HEAD_DIM, seq), BF16),
            pltpu.VMEM((HEAD_DIM, seq), BF16),
            pltpu.VMEM((HEAD_DIM, group * BLK), F32),
            pltpu.VMEM((HEAD_DIM, group * BLK), F32),
        ],
    )
    return pl.pallas_call(
        functools.partial(attn_kernel, group),
        grid_spec=grid_spec,
        out_shape=[
            jax.ShapeDtypeStruct((cols // 2, seq), BF16),
            jax.ShapeDtypeStruct((cols // 2, seq), BF16),
            jax.ShapeDtypeStruct((cols // 2, seq), BF16),
            jax.ShapeDtypeStruct((cols // 2, seq), BF16),
            jax.ShapeDtypeStruct((HEAD_DIM, seq), BF16),
            jax.ShapeDtypeStruct((HEAD_DIM, seq), BF16),
        ],
        compiler_params=pltpu.CompilerParams(dimension_semantics=("arbitrary",), vmem_limit_bytes=56 * 1024 * 1024),
        cost_estimate=pl.CostEstimate(flops=60 * seq * seq * HEAD_DIM, bytes_accessed=12_000_000, transcendentals=group * seq * seq // 2),
        name="attention",
    )(first_blk, packed, packed, packed, packed, starts, cos_t, sin_t)


def assemble_kernel(turn, me_ref, *refs):
    out_ref = refs[-1]
    for rel, ref in enumerate(refs[:-1]):
        tokens = ref.shape[0]
        place = pl.ds(pl.multiple_of((me_ref[0] ^ rel) * tokens, tokens), tokens)
        if turn:
            out_ref[:, place] = ref[...].T
        else:
            out_ref[place, :] = ref[...]


def assemble(pieces, me, turn):
    tokens, width = pieces[0].shape
    seq = tokens * len(pieces)
    col_blk = 512
    if turn:
        out_spec, shape = pl.BlockSpec((col_blk, seq), lambda i, me: (i, 0)), (width, seq)
    else:
        out_spec, shape = pl.BlockSpec((seq, col_blk), lambda i, me: (0, i)), (seq, width)
    return pl.pallas_call(
        functools.partial(assemble_kernel, turn),
        grid_spec=pltpu.PrefetchScalarGridSpec(
            num_scalar_prefetch=1,
            grid=(width // col_blk,),
            in_specs=[pl.BlockSpec((tokens, col_blk), lambda i, me: (0, i)) for _ in pieces],
            out_specs=out_spec,
        ),
        out_shape=jax.ShapeDtypeStruct(shape, BF16),
        compiler_params=pltpu.CompilerParams(dimension_semantics=("arbitrary",), vmem_limit_bytes=32 * 1024 * 1024),
        cost_estimate=pl.CostEstimate(flops=0, bytes_accessed=4 * seq * width, transcendentals=0),
    )(me, *pieces)


def own_kernel(rows, me_ref, *refs):
    out_ref = refs[-1]
    for rel in range(len(refs[:-1]) // len(rows)):
        base = (me_ref[0] ^ rel) * sum(rows)
        for part, height in enumerate(rows):
            place = pl.ds(pl.multiple_of(base + sum(rows[:part]), HALF), height)
            out_ref[place, :] = refs[rel * len(rows) + part][...]


def own_columns(pieces, me, tokens):
    rows = tuple(part.shape[0] for part in pieces[0])
    flat = [part for piece in pieces for part in piece]
    total = sum(rows) * len(pieces)
    return pl.pallas_call(
        functools.partial(own_kernel, rows),
        grid_spec=pltpu.PrefetchScalarGridSpec(
            num_scalar_prefetch=1,
            grid=(1,),
            in_specs=[pl.BlockSpec((part.shape[0], tokens), lambda i, me: (0, me[0])) for part in flat],
            out_specs=pl.BlockSpec((total, tokens), lambda i, me: (0, 0)),
        ),
        out_shape=jax.ShapeDtypeStruct((total, tokens), BF16),
        compiler_params=pltpu.CompilerParams(dimension_semantics=("arbitrary",), vmem_limit_bytes=16 * 1024 * 1024),
        cost_estimate=pl.CostEstimate(flops=0, bytes_accessed=4 * total * tokens, transcendentals=0),
    )(me, *flat)


def wgrad_kernel(by_rows, rels, n_out, me_ref, big_ref, *refs):
    n_in = len(refs) - 3 - n_out
    in_refs, out_refs = refs[:n_in - n_out], refs[n_in:n_in + n_out]
    cat, acc, sems = refs[-3:]
    step, n_steps = pl.program_id(0), pl.num_programs(0)
    slot = lax.rem(step, 2)
    blk = 512
    unit = cat.shape[0] // (len(rels) * n_out)

    def copies(at_step, at_slot):
        out = []
        wide = pl.ds(pl.multiple_of(at_step * blk, blk), blk)
        for o in range(n_out):
            for j, rel in enumerate(rels):
                part = pl.ds((o * len(rels) + j) * unit, unit)
                place = pl.ds(pl.multiple_of((me_ref[0] ^ rel) * unit, unit), unit)
                if by_rows:
                    src, dst = acc.at[at_slot, part, :], out_refs[o].at[place, wide]
                else:
                    src, dst = acc.at[at_slot, :, part], out_refs[o].at[wide, place]
                out.append(pltpu.make_async_copy(src, dst, sems.at[at_slot, o * len(rels) + j]))
        return out

    @pl.when(step == 0)
    def _():
        row = 0
        for ref in in_refs:
            cat[row:row + ref.shape[0], :] = ref[...]
            row += ref.shape[0]

    @pl.when(step >= 2)
    def _():
        for copy in copies(step - 2, slot):
            copy.wait()

    if by_rows:
        acc[slot] = dot_nn(cat[...], big_ref[...])
    else:
        acc[slot] = dot_nt(big_ref[...], cat[...])
    for copy in copies(step, slot):
        copy.start()

    @pl.when(step == n_steps - 1)
    def _():
        for copy in copies(step - 1, 1 - slot):
            copy.wait()
        for copy in copies(step, slot):
            copy.wait()


def weight_grad(big, parts, rels, me, prev, by_rows, n_out, n_dev):
    seq = big.shape[0] if by_rows else big.shape[1]
    width = big.shape[1] if by_rows else big.shape[0]
    rows = sum(part.shape[0] for part in parts)
    unit = rows // (len(rels) * n_out)
    cols = unit * n_dev
    blk = 512
    shape = (cols, width) if by_rows else (width, cols)
    big_spec = pl.BlockSpec((seq, blk), lambda i, me: (0, i)) if by_rows else pl.BlockSpec((blk, seq), lambda i, me: (i, 0))
    acc_shape = (2, rows, blk) if by_rows else (2, blk, rows)
    prev = [] if prev is None else list(prev)
    any_spec = pl.BlockSpec(memory_space=pl.ANY)
    n_fixed = 2 + len(parts)
    body = functools.partial(wgrad_kernel, by_rows, rels, n_out)
    if not prev:
        inner = body
        body = lambda me_ref, big_ref, *refs: inner(me_ref, big_ref, *refs[:len(parts)], *([None] * n_out), *refs[len(parts):])
    return pl.pallas_call(
        body,
        grid_spec=pltpu.PrefetchScalarGridSpec(
            num_scalar_prefetch=1,
            grid=(width // blk,),
            in_specs=[big_spec] + [pl.BlockSpec(part.shape, lambda i, me: (0, 0), pipeline_mode=pl.Buffered(1)) for part in parts] + [any_spec] * len(prev),
            out_specs=[any_spec] * n_out,
            scratch_shapes=[
                pltpu.VMEM((rows, seq), BF16),
                pltpu.VMEM(acc_shape, F32),
                pltpu.SemaphoreType.DMA((2, len(rels) * n_out)),
            ],
        ),
        out_shape=[jax.ShapeDtypeStruct(shape, F32)] * n_out,
        input_output_aliases={n_fixed + o: o for o in range(len(prev))},
        compiler_params=pltpu.CompilerParams(dimension_semantics=("arbitrary",), vmem_limit_bytes=60 * 1024 * 1024),
        cost_estimate=pl.CostEstimate(flops=2 * rows * width * seq, bytes_accessed=4 * width * rows + 2 * seq * (width + rows), transcendentals=0),
    )(me, big, *parts, *prev)


CORE, SIDE_X, SIDE_Y = 1, 2, 4


def solution(mesh):
    n_dev = mesh.shape["sp"]

    def swap(values, bit):
        return lax.ppermute(values, "sp", [(i, i ^ bit) for i in range(n_dev)])

    def reach(first, second):
        return tuple({0: own, SIDE_X: swap(own, SIDE_X), SIDE_Y: swap(own, SIDE_Y)} for own in (first, second))

    def relay(got):
        one, two = got
        one[SIDE_X | SIDE_Y] = swap(one[SIDE_Y], SIDE_X)
        two[SIDE_X | SIDE_Y] = swap(two[SIDE_X], SIDE_Y)
        for part in got:
            for rel in (0, SIDE_X, SIDE_Y):
                part[rel | CORE] = swap(part[rel], CORE)

    def finish(got, dep=None):
        for part in got:
            far = part[SIDE_X | SIDE_Y]
            part[SIDE_X | SIDE_Y | CORE] = swap(far if dep is None else after(far, dep), CORE)

    def after(value, dep):
        return lax.optimization_barrier((value, dep))[0]

    def hold(got, dep):
        for part in got:
            for rel in (SIDE_X, SIDE_Y):
                part[rel] = after(part[rel], dep)

    def device_body(hidden, grad_out, positions, doc_ids, w_q, w_k, w_v, w_o):
        tokens = hidden.shape[0]
        seq = tokens * n_dev
        group = w_q.shape[1] // w_k.shape[1]
        freqs = rope_freqs()
        me = lax.axis_index("sp").astype(jnp.int32)
        me_arr = me[None]
        idx_all = lax.all_gather(jnp.stack([positions, doc_ids])[None], "sp", axis=0, tiled=True)
        idx_all, hidden, grad_out = lax.optimization_barrier((idx_all, hidden, grad_out))
        pos_all = idx_all[:, 0, :].reshape(seq)
        doc_all = idx_all[:, 1, :].reshape(seq)
        starts = jnp.sum((doc_all[None, :] < doc_all[:, None]).astype(jnp.int32), axis=1)
        first_blk = starts[::BLK] // BLK

        angles = positions.astype(F32)[:, None] * freqs[None, :]
        cos_loc, sin_loc = jnp.cos(angles), jnp.sin(angles)
        cos_tab = jnp.concatenate([cos_loc, cos_loc], axis=1)
        sin_tab = jnp.concatenate([-sin_loc, sin_loc], axis=1)
        angles_t = freqs[:, None] * pos_all.astype(F32)[None, :]
        cos_t, sin_t = jnp.cos(angles_t), jnp.sin(angles_t)

        every = tuple(range(n_dev))
        groups = ((0, 1), (2, 3, 4, 5), (6, 7))

        def pairs(got, rels):
            return [half[r] for r in rels for half in got]

        x_got = reach(hidden, grad_out)
        packed = project(hidden, grad_out, w_q, w_k, w_v, w_o, cos_tab, sin_tab, n_dev, group)
        packed = lax.all_to_all(packed, "sp", 0, 0, tiled=True).reshape(seq, -1)
        ctx_lo, ctx_hi, dq_lo, dq_hi, dk_t, dv_t = attention(packed, first_blk, starts[None, :], cos_t, sin_t, group)
        for rel in (SIDE_X, SIDE_Y):
            x_got[1][rel] = after(x_got[1][rel], dk_t)
        relay(x_got)
        kv_got = reach(dk_t, dv_t)
        ctx_got = reach(ctx_lo, ctx_hi)
        dq_got = reach(dq_lo, dq_hi)
        finish(x_got, dk_t)
        x_turned = assemble([x_got[0][r] for r in every], me_arr, True)
        g_all = assemble([x_got[1][r] for r in every], after(me_arr, x_turned), False)
        hold(kv_got, x_turned)
        relay(kv_got)
        (g_q,) = weight_grad(x_turned, pairs(dq_got, (0,)) + [swap(dq_got[0][0], CORE), swap(dq_got[1][0], CORE)], groups[0], after(me_arr, g_all), None, False, 1, n_dev)
        finish(kv_got, g_q)
        g_k, g_v = weight_grad(x_turned, [kv_got[0][r] for r in every] + [kv_got[1][r] for r in every], every, after(me_arr, g_q), None, False, 2, n_dev)
        hold(ctx_got, g_k)
        relay(ctx_got)
        (g_o,) = weight_grad(g_all, pairs(ctx_got, groups[0]), groups[0], after(me_arr, g_k), None, True, 1, n_dev)
        (g_o,) = weight_grad(g_all, pairs(ctx_got, groups[1]), groups[1], me_arr, (g_o,), True, 1, n_dev)
        finish(ctx_got, g_o)
        hold(dq_got, g_o)
        relay(dq_got)
        (g_o,) = weight_grad(g_all, pairs(ctx_got, groups[2]), groups[2], me_arr, (g_o,), True, 1, n_dev)
        own_ctx = own_columns([[half[r] for half in ctx_got] for r in every], after(me_arr, g_o), tokens)
        attn_out = dot_tn(own_ctx, w_o).astype(BF16)
        (g_q,) = weight_grad(x_turned, pairs(dq_got, groups[1]), groups[1], after(me_arr, attn_out), (g_q,), False, 1, n_dev)
        finish(dq_got, g_q)
        (g_q,) = weight_grad(x_turned, pairs(dq_got, groups[2]), groups[2], me_arr, (g_q,), False, 1, n_dev)
        own_k = own_columns([[kv_got[0][r]] for r in every], after(me_arr, g_k), tokens)
        own_v = own_columns([[kv_got[1][r]] for r in every], after(me_arr, g_k), tokens)
        own_q = own_columns([[half[r] for half in dq_got] for r in every], me_arr, tokens)
        grad_hidden = (dot_tt(own_q, w_q) + dot_tt(own_k, w_k) + dot_tt(own_v, w_v)).astype(BF16)
        g_q, g_o = [g_q], [g_o]
        return attn_out, grad_hidden, g_q[0], g_k, g_v, g_o[0]

    tok_spec = P(("dp", "sp"), None)
    vec_spec = P(("dp", "sp"))
    rep_spec = P(None, None)
    part_spec = P("dp", None)
    return jax.shard_map(device_body, mesh=mesh, in_specs=(tok_spec, tok_spec, vec_spec, vec_spec, rep_spec, rep_spec, rep_spec, rep_spec), out_specs=(tok_spec, tok_spec, part_spec, part_spec, part_spec, part_spec), check_vma=False)
```

```python
import functools
import math

import jax
import jax.numpy as jnp
from jax import lax
from jax.experimental import pallas as pl
from jax.experimental.pallas import tpu as pltpu
from jax.sharding import PartitionSpec as P


HEAD_DIM = 128
HALF = HEAD_DIM // 2
ROPE_THETA = 500000.0
ROPE_FACTOR = 8.0
ROPE_LOW = 1.0
ROPE_HIGH = 4.0
ROPE_OLD_CTX = 8192.0
NEG_BIG = -1.0e30
BLK = 256
F32 = jnp.float32
BF16 = jnp.bfloat16


def rope_freqs():
    half_idx = jnp.arange(HALF, dtype=F32)
    inv_freq = jnp.power(ROPE_THETA, -2.0 * half_idx / HEAD_DIM)
    wavelen = 2.0 * jnp.pi / inv_freq
    smooth = (ROPE_OLD_CTX / wavelen - ROPE_LOW) / (ROPE_HIGH - ROPE_LOW)
    mixed_freq = (1.0 - smooth) * inv_freq / ROPE_FACTOR + smooth * inv_freq
    scaled = jnp.where(wavelen > ROPE_OLD_CTX / ROPE_LOW, inv_freq / ROPE_FACTOR, mixed_freq)
    return jnp.where(wavelen < ROPE_OLD_CTX / ROPE_HIGH, inv_freq, scaled)


def dot_nn(lhs, rhs):
    return lax.dot_general(lhs, rhs, (((1,), (0,)), ((), ())), preferred_element_type=F32)


def dot_nt(lhs, rhs):
    return lax.dot_general(lhs, rhs, (((1,), (1,)), ((), ())), preferred_element_type=F32)


def proj_kernel(group, x_ref, g_ref, wq_ref, wk_ref, wv_ref, wo_ref, cos_ref, sin_ref, out_ref):
    cos_tab, sin_tab = cos_ref[...], sin_ref[...]

    def rope(val):
        return (val * cos_tab + pltpu.roll(val, HALF, 1) * sin_tab).astype(BF16)

    width = group * HEAD_DIM
    q_val = dot_nn(x_ref[...], wq_ref[...])
    for head in range(group):
        cols = slice(head * HEAD_DIM, (head + 1) * HEAD_DIM)
        out_ref[0, :, cols] = rope(q_val[:, cols])
    out_ref[0, :, width:2 * width] = dot_nt(g_ref[...], wo_ref[...]).astype(BF16)
    out_ref[0, :, 2 * width:2 * width + HEAD_DIM] = rope(dot_nn(x_ref[...], wk_ref[...]))
    out_ref[0, :, 2 * width + HEAD_DIM:] = dot_nn(x_ref[...], wv_ref[...]).astype(BF16)


def project(hidden, grad_out, w_q, w_k, w_v, w_o, cos_tab, sin_tab, n_dev, group):
    tokens, width = hidden.shape
    cols = group * HEAD_DIM
    total = 2 * cols + 2 * HEAD_DIM
    flops = 2 * tokens * width * n_dev * total
    return pl.pallas_call(
        functools.partial(proj_kernel, group),
        grid=(n_dev,),
        in_specs=[
            pl.BlockSpec((tokens, width), lambda i: (0, 0)),
            pl.BlockSpec((tokens, width), lambda i: (0, 0)),
            pl.BlockSpec((width, cols), lambda i: (0, i)),
            pl.BlockSpec((width, HEAD_DIM), lambda i: (0, i)),
            pl.BlockSpec((width, HEAD_DIM), lambda i: (0, i)),
            pl.BlockSpec((cols, width), lambda i: (i, 0)),
            pl.BlockSpec((tokens, HEAD_DIM), lambda i: (0, 0)),
            pl.BlockSpec((tokens, HEAD_DIM), lambda i: (0, 0)),
        ],
        out_specs=pl.BlockSpec((1, tokens, total), lambda i: (i, 0, 0)),
        out_shape=jax.ShapeDtypeStruct((n_dev, tokens, total), BF16),
        compiler_params=pltpu.CompilerParams(dimension_semantics=("arbitrary",), vmem_limit_bytes=48 * 1024 * 1024),
        cost_estimate=pl.CostEstimate(flops=flops, bytes_accessed=60_000_000, transcendentals=0),
        name="project",
    )(hidden, grad_out, w_q, w_k, w_v, w_o, cos_tab, sin_tab)


def attn_kernel(group, lo_ref, q_ref, do_ref, k_ref, v_ref, start_ref, cos_ref, sin_ref,
                ctx_lo, ctx_hi, dq_lo, dq_hi, dk_ref, dv_ref,
                s_scr, dp_scr, dk_acc, dv_acc, kt_scr, vt_scr, ctx_acc, dq_acc):
    blk = pl.program_id(0)
    n_blk = pl.num_programs(0)
    seq = k_ref.shape[0]
    scale = HEAD_DIM ** -0.5
    exp_scale = scale * math.log2(math.e)

    @pl.when(blk == 0)
    def _():
        dk_acc[...] = jnp.zeros_like(dk_acc)
        dv_acc[...] = jnp.zeros_like(dv_acc)

        @pl.loop(0, seq // BLK)
        def _(c):
            rows = pl.ds(pl.multiple_of(c * BLK, BLK), BLK)
            kt_scr[:, rows] = k_ref[rows, :].astype(F32).T.astype(BF16)
            vt_scr[:, rows] = v_ref[rows, :].astype(F32).T.astype(BF16)

    first = lo_ref[blk]
    last = blk + 1
    heads = [slice(h * HEAD_DIM, (h + 1) * HEAD_DIM) for h in range(group)]
    lanes = [slice(h * BLK, (h + 1) * BLK) for h in range(group)]
    starts = start_ref[...]
    q_idx = blk * BLK + lax.broadcasted_iota(jnp.int32, (1, BLK), 1)
    key_iota = lax.broadcasted_iota(jnp.int32, (BLK, BLK), 0)

    def score_step(c, peaks):
        rows = pl.ds(pl.multiple_of(c * BLK, BLK), BLK)
        key_idx = key_iota + c * BLK
        allowed = (key_idx >= starts) & (key_idx <= q_idx)
        k_blk = k_ref[rows, :]
        out = []
        for h in range(group):
            scores = jnp.where(allowed, dot_nt(k_blk, q_ref[:, heads[h]]), NEG_BIG)
            s_scr[rows, lanes[h]] = scores
            out.append(jnp.maximum(peaks[h], jnp.max(scores, axis=0, keepdims=True)))
        return tuple(out)

    peaks = lax.fori_loop(first, last, score_step, tuple(jnp.full((1, BLK), NEG_BIG, F32) for _ in range(group)))
    peaks = tuple(peak * exp_scale for peak in peaks)

    def exp_step(c, sums):
        rows = pl.ds(pl.multiple_of(c * BLK, BLK), BLK)
        v_blk = v_ref[rows, :]
        out = []
        for h in range(group):
            probs = jnp.exp2(s_scr[rows, lanes[h]] * exp_scale - peaks[h])
            d_prob = dot_nt(v_blk, do_ref[:, heads[h]])
            s_scr[rows, lanes[h]] = probs
            dp_scr[rows, lanes[h]] = d_prob
            out.append(sums[2 * h] + jnp.sum(probs, axis=0, keepdims=True))
            out.append(sums[2 * h + 1] + jnp.sum(probs * d_prob, axis=0, keepdims=True))
        return tuple(out)

    sums = lax.fori_loop(first, last, exp_step, tuple(jnp.zeros((1, BLK), F32) for _ in range(2 * group)))
    inv_sum = [1.0 / sums[2 * h] for h in range(group)]
    row_dot = [sums[2 * h + 1] * inv_sum[h] for h in range(group)]

    ctx_acc[...] = jnp.zeros_like(ctx_acc)
    dq_acc[...] = jnp.zeros_like(dq_acc)

    def grad_step(c, carry):
        rows = pl.ds(pl.multiple_of(c * BLK, BLK), BLK)
        k_t, v_t = kt_scr[:, rows], vt_scr[:, rows]
        dk_sum, dv_sum = dk_acc[rows, :], dv_acc[rows, :]
        for h in range(group):
            probs = s_scr[rows, lanes[h]] * inv_sum[h]
            probs_bf = probs.astype(BF16)
            d_score = (probs * (dp_scr[rows, lanes[h]] - row_dot[h]) * scale).astype(BF16)
            ctx_acc[:, lanes[h]] += dot_nn(v_t, probs_bf)
            dq_acc[:, lanes[h]] += dot_nn(k_t, d_score)
            dk_sum = dk_sum + dot_nn(d_score, q_ref[:, heads[h]])
            dv_sum = dv_sum + dot_nn(probs_bf, do_ref[:, heads[h]])
        dk_acc[rows, :] = dk_sum
        dv_acc[rows, :] = dv_sum
        return carry

    lax.fori_loop(first, last, grad_step, 0)

    def unrope(val, cos_tab, sin_tab):
        upper, lower = val[:HALF], val[HALF:]
        return (upper * cos_tab + lower * sin_tab).astype(BF16), (lower * cos_tab - upper * sin_tab).astype(BF16)

    own = pl.ds(pl.multiple_of(blk * BLK, BLK), BLK)
    cos_q, sin_q = cos_ref[:, own], sin_ref[:, own]
    half = ctx_lo.shape[0]
    for h in range(group):
        ctx_val = ctx_acc[:, lanes[h]].astype(BF16)
        dq_val = unrope(dq_acc[:, lanes[h]].astype(BF16).astype(F32), cos_q, sin_q)
        for part in range(2):
            row = h * HEAD_DIM + part * HALF
            ctx_out, dq_out = (ctx_lo, dq_lo) if row < half else (ctx_hi, dq_hi)
            place = slice(row % half, row % half + HALF)
            ctx_out[place, :] = ctx_val[part * HALF:(part + 1) * HALF]
            dq_out[place, :] = dq_val[part]

    @pl.when(blk == n_blk - 1)
    def _():
        @pl.loop(0, seq // BLK)
        def _(c):
            rows = pl.ds(pl.multiple_of(c * BLK, BLK), BLK)
            upper, lower = unrope(dk_acc[rows, :].T.astype(BF16).astype(F32), cos_ref[:, rows], sin_ref[:, rows])
            dk_ref[:HALF, rows] = upper
            dk_ref[HALF:, rows] = lower
            dv_ref[:, rows] = dv_acc[rows, :].T.astype(BF16)


def attention(packed, first_blk, starts, cos_t, sin_t, group):
    seq = packed.shape[0]
    cols = group * HEAD_DIM
    n_blk = seq // BLK
    grid_spec = pltpu.PrefetchScalarGridSpec(
        num_scalar_prefetch=1,
        grid=(n_blk,),
        in_specs=[
            pl.BlockSpec((BLK, cols), lambda i, lo: (i, 0)),
            pl.BlockSpec((BLK, cols), lambda i, lo: (i, 1)),
            pl.BlockSpec((seq, HEAD_DIM), lambda i, lo: (0, 2 * group)),
            pl.BlockSpec((seq, HEAD_DIM), lambda i, lo: (0, 2 * group + 1)),
            pl.BlockSpec((1, BLK), lambda i, lo: (0, i)),
            pl.BlockSpec((HALF, seq), lambda i, lo: (0, 0)),
            pl.BlockSpec((HALF, seq), lambda i, lo: (0, 0)),
        ],
        out_specs=[
            pl.BlockSpec((cols // 2, BLK), lambda i, lo: (0, i)),
            pl.BlockSpec((cols // 2, BLK), lambda i, lo: (0, i)),
            pl.BlockSpec((cols // 2, BLK), lambda i, lo: (0, i)),
            pl.BlockSpec((cols // 2, BLK), lambda i, lo: (0, i)),
            pl.BlockSpec((HEAD_DIM, seq), lambda i, lo: (0, 0)),
            pl.BlockSpec((HEAD_DIM, seq), lambda i, lo: (0, 0)),
        ],
        scratch_shapes=[
            pltpu.VMEM((seq, group * BLK), F32),
            pltpu.VMEM((seq, group * BLK), F32),
            pltpu.VMEM((seq, HEAD_DIM), F32),
            pltpu.VMEM((seq, HEAD_DIM), F32),
            pltpu.VMEM((HEAD_DIM, seq), BF16),
            pltpu.VMEM((HEAD_DIM, seq), BF16),
            pltpu.VMEM((HEAD_DIM, group * BLK), F32),
            pltpu.VMEM((HEAD_DIM, group * BLK), F32),
        ],
    )
    return pl.pallas_call(
        functools.partial(attn_kernel, group),
        grid_spec=grid_spec,
        out_shape=[
            jax.ShapeDtypeStruct((cols // 2, seq), BF16),
            jax.ShapeDtypeStruct((cols // 2, seq), BF16),
            jax.ShapeDtypeStruct((cols // 2, seq), BF16),
            jax.ShapeDtypeStruct((cols // 2, seq), BF16),
            jax.ShapeDtypeStruct((HEAD_DIM, seq), BF16),
            jax.ShapeDtypeStruct((HEAD_DIM, seq), BF16),
        ],
        compiler_params=pltpu.CompilerParams(dimension_semantics=("arbitrary",), vmem_limit_bytes=56 * 1024 * 1024),
        cost_estimate=pl.CostEstimate(flops=60 * seq * seq * HEAD_DIM, bytes_accessed=12_000_000, transcendentals=group * seq * seq // 2),
        name="attention",
    )(first_blk, packed, packed, packed, packed, starts, cos_t, sin_t)


def assemble_kernel(turn, half_steps, me_ref, *refs):
    out_ref = refs[-1]
    n_dev = len(refs) // 2

    def fill(ins):
        for rel, ref in enumerate(ins):
            tokens = ref.shape[0]
            place = pl.ds(pl.multiple_of((me_ref[0] ^ rel) * tokens, tokens), tokens)
            if turn:
                out_ref[:, place] = ref[...].T
            else:
                out_ref[place, :] = ref[...]

    @pl.when(pl.program_id(0) < half_steps)
    def _():
        fill(refs[:n_dev])

    @pl.when(pl.program_id(0) >= half_steps)
    def _():
        fill(refs[n_dev:2 * n_dev])


def assemble(low, high, me, turn):
    tokens, half_width = low[0].shape
    seq, width = tokens * len(low), 2 * half_width
    col_blk = 512
    steps = half_width // col_blk
    if turn:
        out_spec, shape = pl.BlockSpec((col_blk, seq), lambda i, me: (i, 0)), (width, seq)
    else:
        out_spec, shape = pl.BlockSpec((seq, col_blk), lambda i, me: (0, i)), (seq, width)
    low_specs = [pl.BlockSpec((tokens, col_blk), lambda i, me: (0, jnp.minimum(i, steps - 1))) for _ in low]
    high_specs = [pl.BlockSpec((tokens, col_blk), lambda i, me: (0, jnp.maximum(i - steps, 0))) for _ in high]
    return pl.pallas_call(
        functools.partial(assemble_kernel, turn, steps),
        grid_spec=pltpu.PrefetchScalarGridSpec(
            num_scalar_prefetch=1,
            grid=(2 * steps,),
            in_specs=low_specs + high_specs,
            out_specs=out_spec,
        ),
        out_shape=jax.ShapeDtypeStruct(shape, BF16),
        compiler_params=pltpu.CompilerParams(dimension_semantics=("arbitrary",), vmem_limit_bytes=28 * 1024 * 1024),
        cost_estimate=pl.CostEstimate(flops=0, bytes_accessed=4 * seq * width, transcendentals=0),
    )(me, *low, *high)


def own_kernel(kinds, turned, me_ref, *refs):
    n_parts = sum(len(rows) * count for rows, count in kinds)
    parts, weights, (out_ref, scr) = refs[:n_parts], refs[n_parts:-2], refs[-2:]

    @pl.when(pl.program_id(0) == 0)
    def _():
        at = start = 0
        for rows, count in kinds:
            unit = sum(rows)
            for rel in range(count):
                block = jnp.concatenate([parts[at + j][...] for j in range(len(rows))], axis=0)
                at += len(rows)
                place = pl.ds(pl.multiple_of(start + (me_ref[0] ^ rel) * unit, HEAD_DIM), unit)
                scr[:, place] = block.T
            start += unit * count

    total = None
    start = 0
    for (rows, count), weight in zip(kinds, weights):
        width = sum(rows) * count
        dot = dot_nt if turned else dot_nn
        term = dot(scr[:, start:start + width], weight[...])
        total = term if total is None else total + term
        start += width
    out_ref[...] = total.astype(BF16)


def own_product(groups, weights, me, tokens, turned):
    kinds = tuple((tuple(part.shape[0] for part in pieces[0]), len(pieces)) for pieces in groups)
    flat = [part for pieces in groups for piece in pieces for part in piece]
    width = weights[0].shape[0] if turned else weights[0].shape[1]
    depth = sum(sum(rows) * count for rows, count in kinds)
    blk = 512
    if turned:
        weight_specs = [pl.BlockSpec((blk, weight.shape[1]), lambda i, me: (i, 0)) for weight in weights]
    else:
        weight_specs = [pl.BlockSpec((weight.shape[0], blk), lambda i, me: (0, i)) for weight in weights]
    return pl.pallas_call(
        functools.partial(own_kernel, kinds, turned),
        grid_spec=pltpu.PrefetchScalarGridSpec(
            num_scalar_prefetch=1,
            grid=(width // blk,),
            in_specs=[pl.BlockSpec((part.shape[0], tokens), lambda i, me: (0, me[0]), pipeline_mode=pl.Buffered(1)) for part in flat] + weight_specs,
            out_specs=pl.BlockSpec((tokens, blk), lambda i, me: (0, i)),
            scratch_shapes=[pltpu.VMEM((tokens, depth), BF16)],
        ),
        out_shape=jax.ShapeDtypeStruct((tokens, width), BF16),
        compiler_params=pltpu.CompilerParams(dimension_semantics=("arbitrary",), vmem_limit_bytes=32 * 1024 * 1024),
        cost_estimate=pl.CostEstimate(flops=2 * tokens * width * depth, bytes_accessed=2 * depth * (width + tokens), transcendentals=0),
    )(me, *flat, *weights)


def wgrad_kernel(by_rows, rels, n_out, me_ref, big_ref, *refs):
    n_in = len(refs) - 3 - n_out
    in_refs, out_refs = refs[:n_in - n_out], refs[n_in:n_in + n_out]
    cat, acc, sems = refs[-3:]
    step, n_steps = pl.program_id(0), pl.num_programs(0)
    slot = lax.rem(step, 2)
    blk = 512
    unit = cat.shape[0] // (len(rels) * n_out)

    def copies(at_step, at_slot):
        out = []
        wide = pl.ds(pl.multiple_of(at_step * blk, blk), blk)
        for o in range(n_out):
            for j, rel in enumerate(rels):
                part = pl.ds((o * len(rels) + j) * unit, unit)
                place = pl.ds(pl.multiple_of((me_ref[0] ^ rel) * unit, unit), unit)
                if by_rows:
                    src, dst = acc.at[at_slot, part, :], out_refs[o].at[place, wide]
                else:
                    src, dst = acc.at[at_slot, :, part], out_refs[o].at[wide, place]
                out.append(pltpu.make_async_copy(src, dst, sems.at[at_slot, o * len(rels) + j]))
        return out

    @pl.when(step == 0)
    def _():
        row = 0
        for ref in in_refs:
            cat[row:row + ref.shape[0], :] = ref[...]
            row += ref.shape[0]

    @pl.when(step >= 2)
    def _():
        for copy in copies(step - 2, slot):
            copy.wait()

    if by_rows:
        acc[slot] = dot_nn(cat[...], big_ref[...])
    else:
        acc[slot] = dot_nt(big_ref[...], cat[...])
    for copy in copies(step, slot):
        copy.start()

    @pl.when(step == n_steps - 1)
    def _():
        for copy in copies(step - 1, 1 - slot):
            copy.wait()
        for copy in copies(step, slot):
            copy.wait()


def weight_grad(big, parts, rels, me, prev, by_rows, n_out, n_dev):
    seq = big.shape[0] if by_rows else big.shape[1]
    width = big.shape[1] if by_rows else big.shape[0]
    rows = sum(part.shape[0] for part in parts)
    unit = rows // (len(rels) * n_out)
    cols = unit * n_dev
    blk = 512
    shape = (cols, width) if by_rows else (width, cols)
    big_spec = pl.BlockSpec((seq, blk), lambda i, me: (0, i)) if by_rows else pl.BlockSpec((blk, seq), lambda i, me: (i, 0))
    acc_shape = (2, rows, blk) if by_rows else (2, blk, rows)
    prev = [] if prev is None else list(prev)
    any_spec = pl.BlockSpec(memory_space=pl.ANY)
    n_fixed = 2 + len(parts)
    body = functools.partial(wgrad_kernel, by_rows, rels, n_out)
    if not prev:
        inner = body
        body = lambda me_ref, big_ref, *refs: inner(me_ref, big_ref, *refs[:len(parts)], *([None] * n_out), *refs[len(parts):])
    return pl.pallas_call(
        body,
        grid_spec=pltpu.PrefetchScalarGridSpec(
            num_scalar_prefetch=1,
            grid=(width // blk,),
            in_specs=[big_spec] + [pl.BlockSpec(part.shape, lambda i, me: (0, 0), pipeline_mode=pl.Buffered(1)) for part in parts] + [any_spec] * len(prev),
            out_specs=[any_spec] * n_out,
            scratch_shapes=[
                pltpu.VMEM((rows, seq), BF16),
                pltpu.VMEM(acc_shape, F32),
                pltpu.SemaphoreType.DMA((2, len(rels) * n_out)),
            ],
        ),
        out_shape=[jax.ShapeDtypeStruct(shape, F32)] * n_out,
        input_output_aliases={n_fixed + o: o for o in range(len(prev))},
        compiler_params=pltpu.CompilerParams(dimension_semantics=("arbitrary",), vmem_limit_bytes=48 * 1024 * 1024),
        cost_estimate=pl.CostEstimate(flops=2 * rows * width * seq, bytes_accessed=4 * width * rows + 2 * seq * (width + rows), transcendentals=0),
    )(me, big, *parts, *prev)


CORE, SIDE_X, SIDE_Y = 1, 2, 4


def solution(mesh):
    n_dev = mesh.shape["sp"]

    def swap(values, bit):
        return lax.ppermute(values, "sp", [(i, i ^ bit) for i in range(n_dev)])

    def reach(first, second):
        return tuple({0: own, SIDE_X: swap(own, SIDE_X), SIDE_Y: swap(own, SIDE_Y)} for own in (first, second))

    def relay(got):
        one, two = got
        one[SIDE_X | SIDE_Y] = swap(one[SIDE_Y], SIDE_X)
        two[SIDE_X | SIDE_Y] = swap(two[SIDE_X], SIDE_Y)
        for part in got:
            for rel in (0, SIDE_X, SIDE_Y):
                part[rel | CORE] = swap(part[rel], CORE)

    def finish(got, dep=None):
        for part in got:
            far = part[SIDE_X | SIDE_Y]
            part[SIDE_X | SIDE_Y | CORE] = swap(far if dep is None else after(far, dep), CORE)

    def after(value, dep):
        return lax.optimization_barrier((value, dep))[0]

    def hold(got, dep):
        for part in got:
            for rel in (SIDE_X, SIDE_Y):
                part[rel] = after(part[rel], dep)

    def device_body(hidden, grad_out, positions, doc_ids, w_q, w_k, w_v, w_o):
        tokens = hidden.shape[0]
        seq = tokens * n_dev
        group = w_q.shape[1] // w_k.shape[1]
        freqs = rope_freqs()
        me = lax.axis_index("sp").astype(jnp.int32)
        me_arr = me[None]
        idx = {0: jnp.stack([positions, doc_ids])}
        idx[SIDE_X], idx[SIDE_Y] = swap(idx[0], SIDE_X), swap(idx[0], SIDE_Y)
        idx[SIDE_X | SIDE_Y] = swap(idx[0], SIDE_X | SIDE_Y)
        for rel in (0, SIDE_X, SIDE_Y, SIDE_X | SIDE_Y):
            idx[rel | CORE] = swap(idx[0], rel | CORE)
        order = me ^ jnp.arange(n_dev, dtype=jnp.int32)
        idx_all = jnp.take(jnp.stack([idx[rel] for rel in range(n_dev)]), order, axis=0)
        pos_all = idx_all[:, 0, :].reshape(seq)
        doc_all = idx_all[:, 1, :].reshape(seq)
        starts = jnp.sum((doc_all[None, :] < doc_all[:, None]).astype(jnp.int32), axis=1)
        first_blk = starts[::BLK] // BLK

        angles = positions.astype(F32)[:, None] * freqs[None, :]
        cos_loc, sin_loc = jnp.cos(angles), jnp.sin(angles)
        cos_tab = jnp.concatenate([cos_loc, cos_loc], axis=1)
        sin_tab = jnp.concatenate([-sin_loc, sin_loc], axis=1)
        angles_t = freqs[:, None] * pos_all.astype(F32)[None, :]
        cos_t, sin_t = jnp.cos(angles_t), jnp.sin(angles_t)

        every = tuple(range(n_dev))
        groups = ((0, 1), (2, 3, 4, 5), (6, 7))

        def pairs(got, rels):
            return [half[r] for r in rels for half in got]

        half = hidden.shape[1] // 2
        x_got = reach(hidden[:, :half], hidden[:, half:])
        packed = project(hidden, grad_out, w_q, w_k, w_v, w_o, cos_tab, sin_tab, n_dev, group)
        packed = lax.all_to_all(packed, "sp", 0, 0, tiled=True).reshape(seq, -1)
        relay(x_got)
        g_got = reach(grad_out[:, :half], grad_out[:, half:])
        ctx_lo, ctx_hi, dq_lo, dq_hi, dk_t, dv_t = attention(packed, first_blk, starts[None, :], cos_t, sin_t, group)
        finish(x_got, dk_t)
        kv_got = reach(dk_t, dv_t)
        ctx_got = reach(ctx_lo, ctx_hi)
        dq_got = reach(dq_lo, dq_hi)

        x_turned = assemble([x_got[0][r] for r in every], [x_got[1][r] for r in every], after(me_arr, dk_t), True)
        hold(g_got, x_turned)
        relay(g_got)
        (g_q,) = weight_grad(x_turned, pairs(dq_got, (0,)) + [swap(dq_got[0][0], CORE), swap(dq_got[1][0], CORE)], groups[0], me_arr, None, False, 1, n_dev)
        finish(g_got, g_q)
        g_all = assemble([g_got[0][r] for r in every], [g_got[1][r] for r in every], after(me_arr, g_q), False)
        (g_o,) = weight_grad(g_all, pairs(ctx_got, (0,)) + [swap(ctx_got[0][0], CORE), swap(ctx_got[1][0], CORE)], groups[0], me_arr, None, True, 1, n_dev)
        hold(ctx_got, g_o)
        relay(ctx_got)
        (g_o,) = weight_grad(g_all, pairs(ctx_got, groups[1]), groups[1], me_arr, (g_o,), True, 1, n_dev)
        finish(ctx_got, g_o)
        (g_o,) = weight_grad(g_all, pairs(ctx_got, groups[2]), groups[2], me_arr, (g_o,), True, 1, n_dev)
        hold(kv_got, g_o)
        relay(kv_got)
        attn_out = own_product([[[part[r] for part in ctx_got] for r in every]], [w_o], after(me_arr, g_o), tokens, False)
        finish(kv_got, attn_out)
        g_k, g_v = weight_grad(x_turned, [kv_got[0][r] for r in every] + [kv_got[1][r] for r in every], every, after(me_arr, attn_out), None, False, 2, n_dev)
        hold(dq_got, g_k)
        relay(dq_got)
        (g_q,) = weight_grad(x_turned, pairs(dq_got, groups[1]), groups[1], after(me_arr, g_k), (g_q,), False, 1, n_dev)
        finish(dq_got, g_q)
        (g_q,) = weight_grad(x_turned, pairs(dq_got, groups[2]), groups[2], me_arr, (g_q,), False, 1, n_dev)
        sources = [[[part[r] for part in dq_got] for r in every], [[kv_got[0][r]] for r in every], [[kv_got[1][r]] for r in every]]
        grad_hidden = own_product(sources, [w_q, w_k, w_v], after(me_arr, g_q), tokens, True)
        return attn_out, grad_hidden, g_q, g_k, g_v, g_o

    tok_spec = P(("dp", "sp"), None)
    vec_spec = P(("dp", "sp"))
    rep_spec = P(None, None)
    part_spec = P("dp", None)
    return jax.shard_map(device_body, mesh=mesh, in_specs=(tok_spec, tok_spec, vec_spec, vec_spec, rep_spec, rep_spec, rep_spec, rep_spec), out_specs=(tok_spec, tok_spec, part_spec, part_spec, part_spec, part_spec), check_vma=False)
```

```python
import functools
import math

import jax
import jax.numpy as jnp
from jax import lax
from jax.experimental import pallas as pl
from jax.experimental.pallas import tpu as pltpu
from jax.sharding import PartitionSpec as P


HEAD_DIM = 128
HALF = HEAD_DIM // 2
ROPE_THETA = 500000.0
ROPE_FACTOR = 8.0
ROPE_LOW = 1.0
ROPE_HIGH = 4.0
ROPE_OLD_CTX = 8192.0
NEG_BIG = -1.0e30
BLK = 256
F32 = jnp.float32
BF16 = jnp.bfloat16


def rope_freqs():
    half_idx = jnp.arange(HALF, dtype=F32)
    inv_freq = jnp.power(ROPE_THETA, -2.0 * half_idx / HEAD_DIM)
    wavelen = 2.0 * jnp.pi / inv_freq
    smooth = (ROPE_OLD_CTX / wavelen - ROPE_LOW) / (ROPE_HIGH - ROPE_LOW)
    mixed_freq = (1.0 - smooth) * inv_freq / ROPE_FACTOR + smooth * inv_freq
    scaled = jnp.where(wavelen > ROPE_OLD_CTX / ROPE_LOW, inv_freq / ROPE_FACTOR, mixed_freq)
    return jnp.where(wavelen < ROPE_OLD_CTX / ROPE_HIGH, inv_freq, scaled)


def dot_nn(lhs, rhs):
    return lax.dot_general(lhs, rhs, (((1,), (0,)), ((), ())), preferred_element_type=F32)


def dot_nt(lhs, rhs):
    return lax.dot_general(lhs, rhs, (((1,), (1,)), ((), ())), preferred_element_type=F32)


def proj_kernel(group, x_ref, g_ref, wq_ref, wk_ref, wv_ref, wo_ref, cos_ref, sin_ref, out_ref):
    cos_tab, sin_tab = cos_ref[...], sin_ref[...]

    def rope(val):
        return (val * cos_tab + pltpu.roll(val, HALF, 1) * sin_tab).astype(BF16)

    width = group * HEAD_DIM
    q_val = dot_nn(x_ref[...], wq_ref[...])
    for head in range(group):
        cols = slice(head * HEAD_DIM, (head + 1) * HEAD_DIM)
        out_ref[0, :, cols] = rope(q_val[:, cols])
    out_ref[0, :, width:2 * width] = dot_nt(g_ref[...], wo_ref[...]).astype(BF16)
    out_ref[0, :, 2 * width:2 * width + HEAD_DIM] = rope(dot_nn(x_ref[...], wk_ref[...]))
    out_ref[0, :, 2 * width + HEAD_DIM:] = dot_nn(x_ref[...], wv_ref[...]).astype(BF16)


def project(hidden, grad_out, w_q, w_k, w_v, w_o, cos_tab, sin_tab, n_dev, group):
    tokens, width = hidden.shape
    cols = group * HEAD_DIM
    total = 2 * cols + 2 * HEAD_DIM
    flops = 2 * tokens * width * n_dev * total
    return pl.pallas_call(
        functools.partial(proj_kernel, group),
        grid=(n_dev,),
        in_specs=[
            pl.BlockSpec((tokens, width), lambda i: (0, 0)),
            pl.BlockSpec((tokens, width), lambda i: (0, 0)),
            pl.BlockSpec((width, cols), lambda i: (0, i)),
            pl.BlockSpec((width, HEAD_DIM), lambda i: (0, i)),
            pl.BlockSpec((width, HEAD_DIM), lambda i: (0, i)),
            pl.BlockSpec((cols, width), lambda i: (i, 0)),
            pl.BlockSpec((tokens, HEAD_DIM), lambda i: (0, 0)),
            pl.BlockSpec((tokens, HEAD_DIM), lambda i: (0, 0)),
        ],
        out_specs=pl.BlockSpec((1, tokens, total), lambda i: (i, 0, 0)),
        out_shape=jax.ShapeDtypeStruct((n_dev, tokens, total), BF16),
        compiler_params=pltpu.CompilerParams(dimension_semantics=("arbitrary",), vmem_limit_bytes=60 * 1024 * 1024),
        cost_estimate=pl.CostEstimate(flops=flops, bytes_accessed=60_000_000, transcendentals=0),
        name="project",
    )(hidden, grad_out, w_q, w_k, w_v, w_o, cos_tab, sin_tab)


def attn_kernel(group, lo_ref, q_ref, do_ref, k_ref, v_ref, start_ref, cos_ref, sin_ref,
                ctx_lo, ctx_hi, dq_lo, dq_hi, dk_ref, dv_ref,
                s_scr, dp_scr, dk_acc, dv_acc, kt_scr, vt_scr, ctx_acc, dq_acc):
    blk = pl.program_id(0)
    n_blk = pl.num_programs(0)
    seq = k_ref.shape[0]
    scale = HEAD_DIM ** -0.5
    exp_scale = scale * math.log2(math.e)

    @pl.when(blk == 0)
    def _():
        dk_acc[...] = jnp.zeros_like(dk_acc)
        dv_acc[...] = jnp.zeros_like(dv_acc)

        @pl.loop(0, seq // BLK)
        def _(c):
            rows = pl.ds(pl.multiple_of(c * BLK, BLK), BLK)
            kt_scr[:, rows] = k_ref[rows, :].astype(F32).T.astype(BF16)
            vt_scr[:, rows] = v_ref[rows, :].astype(F32).T.astype(BF16)

    first = lo_ref[blk]
    last = blk + 1
    heads = [slice(h * HEAD_DIM, (h + 1) * HEAD_DIM) for h in range(group)]
    lanes = [slice(h * BLK, (h + 1) * BLK) for h in range(group)]
    starts = start_ref[...]
    q_idx = blk * BLK + lax.broadcasted_iota(jnp.int32, (1, BLK), 1)
    key_iota = lax.broadcasted_iota(jnp.int32, (BLK, BLK), 0)

    def score_step(c, peaks):
        rows = pl.ds(pl.multiple_of(c * BLK, BLK), BLK)
        key_idx = key_iota + c * BLK
        allowed = (key_idx >= starts) & (key_idx <= q_idx)
        k_blk = k_ref[rows, :]
        out = []
        for h in range(group):
            scores = jnp.where(allowed, dot_nt(k_blk, q_ref[:, heads[h]]), NEG_BIG)
            s_scr[rows, lanes[h]] = scores
            out.append(jnp.maximum(peaks[h], jnp.max(scores, axis=0, keepdims=True)))
        return tuple(out)

    peaks = lax.fori_loop(first, last, score_step, tuple(jnp.full((1, BLK), NEG_BIG, F32) for _ in range(group)))
    peaks = tuple(peak * exp_scale for peak in peaks)

    def exp_step(c, sums):
        rows = pl.ds(pl.multiple_of(c * BLK, BLK), BLK)
        v_blk = v_ref[rows, :]
        out = []
        for h in range(group):
            probs = jnp.exp2(s_scr[rows, lanes[h]] * exp_scale - peaks[h])
            d_prob = dot_nt(v_blk, do_ref[:, heads[h]])
            s_scr[rows, lanes[h]] = probs
            dp_scr[rows, lanes[h]] = d_prob
            out.append(sums[2 * h] + jnp.sum(probs, axis=0, keepdims=True))
            out.append(sums[2 * h + 1] + jnp.sum(probs * d_prob, axis=0, keepdims=True))
        return tuple(out)

    sums = lax.fori_loop(first, last, exp_step, tuple(jnp.zeros((1, BLK), F32) for _ in range(2 * group)))
    inv_sum = [1.0 / sums[2 * h] for h in range(group)]
    row_dot = [sums[2 * h + 1] * inv_sum[h] for h in range(group)]

    ctx_acc[...] = jnp.zeros_like(ctx_acc)
    dq_acc[...] = jnp.zeros_like(dq_acc)

    def grad_step(c, carry):
        rows = pl.ds(pl.multiple_of(c * BLK, BLK), BLK)
        k_t, v_t = kt_scr[:, rows], vt_scr[:, rows]
        dk_sum, dv_sum = dk_acc[rows, :], dv_acc[rows, :]
        for h in range(group):
            probs = s_scr[rows, lanes[h]] * inv_sum[h]
            probs_bf = probs.astype(BF16)
            d_score = (probs * (dp_scr[rows, lanes[h]] - row_dot[h]) * scale).astype(BF16)
            ctx_acc[:, lanes[h]] += dot_nn(v_t, probs_bf)
            dq_acc[:, lanes[h]] += dot_nn(k_t, d_score)
            dk_sum = dk_sum + dot_nn(d_score, q_ref[:, heads[h]])
            dv_sum = dv_sum + dot_nn(probs_bf, do_ref[:, heads[h]])
        dk_acc[rows, :] = dk_sum
        dv_acc[rows, :] = dv_sum
        return carry

    lax.fori_loop(first, last, grad_step, 0)

    def unrope(val, cos_tab, sin_tab):
        upper, lower = val[:HALF], val[HALF:]
        return (upper * cos_tab + lower * sin_tab).astype(BF16), (lower * cos_tab - upper * sin_tab).astype(BF16)

    own = pl.ds(pl.multiple_of(blk * BLK, BLK), BLK)
    cos_q, sin_q = cos_ref[:, own], sin_ref[:, own]
    half = ctx_lo.shape[0]
    for h in range(group):
        ctx_val = ctx_acc[:, lanes[h]].astype(BF16)
        dq_val = unrope(dq_acc[:, lanes[h]].astype(BF16).astype(F32), cos_q, sin_q)
        for part in range(2):
            row = h * HEAD_DIM + part * HALF
            ctx_out, dq_out = (ctx_lo, dq_lo) if row < half else (ctx_hi, dq_hi)
            place = slice(row % half, row % half + HALF)
            ctx_out[place, :] = ctx_val[part * HALF:(part + 1) * HALF]
            dq_out[place, :] = dq_val[part]

    @pl.when(blk == n_blk - 1)
    def _():
        @pl.loop(0, seq // BLK)
        def _(c):
            rows = pl.ds(pl.multiple_of(c * BLK, BLK), BLK)
            upper, lower = unrope(dk_acc[rows, :].T.astype(BF16).astype(F32), cos_ref[:, rows], sin_ref[:, rows])
            dk_ref[:HALF, rows] = upper
            dk_ref[HALF:, rows] = lower
            dv_ref[:, rows] = dv_acc[rows, :].T.astype(BF16)


def attention(packed, first_blk, starts, cos_t, sin_t, group):
    seq = packed.shape[0]
    cols = group * HEAD_DIM
    n_blk = seq // BLK
    grid_spec = pltpu.PrefetchScalarGridSpec(
        num_scalar_prefetch=1,
        grid=(n_blk,),
        in_specs=[
            pl.BlockSpec((BLK, cols), lambda i, lo: (i, 0)),
            pl.BlockSpec((BLK, cols), lambda i, lo: (i, 1)),
            pl.BlockSpec((seq, HEAD_DIM), lambda i, lo: (0, 2 * group)),
            pl.BlockSpec((seq, HEAD_DIM), lambda i, lo: (0, 2 * group + 1)),
            pl.BlockSpec((1, BLK), lambda i, lo: (0, i)),
            pl.BlockSpec((HALF, seq), lambda i, lo: (0, 0)),
            pl.BlockSpec((HALF, seq), lambda i, lo: (0, 0)),
        ],
        out_specs=[
            pl.BlockSpec((cols // 2, BLK), lambda i, lo: (0, i)),
            pl.BlockSpec((cols // 2, BLK), lambda i, lo: (0, i)),
            pl.BlockSpec((cols // 2, BLK), lambda i, lo: (0, i)),
            pl.BlockSpec((cols // 2, BLK), lambda i, lo: (0, i)),
            pl.BlockSpec((HEAD_DIM, seq), lambda i, lo: (0, 0)),
            pl.BlockSpec((HEAD_DIM, seq), lambda i, lo: (0, 0)),
        ],
        scratch_shapes=[
            pltpu.VMEM((seq, group * BLK), F32),
            pltpu.VMEM((seq, group * BLK), F32),
            pltpu.VMEM((seq, HEAD_DIM), F32),
            pltpu.VMEM((seq, HEAD_DIM), F32),
            pltpu.VMEM((HEAD_DIM, seq), BF16),
            pltpu.VMEM((HEAD_DIM, seq), BF16),
            pltpu.VMEM((HEAD_DIM, group * BLK), F32),
            pltpu.VMEM((HEAD_DIM, group * BLK), F32),
        ],
    )
    return pl.pallas_call(
        functools.partial(attn_kernel, group),
        grid_spec=grid_spec,
        out_shape=[
            jax.ShapeDtypeStruct((cols // 2, seq), BF16),
            jax.ShapeDtypeStruct((cols // 2, seq), BF16),
            jax.ShapeDtypeStruct((cols // 2, seq), BF16),
            jax.ShapeDtypeStruct((cols // 2, seq), BF16),
            jax.ShapeDtypeStruct((HEAD_DIM, seq), BF16),
            jax.ShapeDtypeStruct((HEAD_DIM, seq), BF16),
        ],
        compiler_params=pltpu.CompilerParams(dimension_semantics=("arbitrary",), vmem_limit_bytes=56 * 1024 * 1024),
        cost_estimate=pl.CostEstimate(flops=60 * seq * seq * HEAD_DIM, bytes_accessed=12_000_000, transcendentals=group * seq * seq // 2),
        name="attention",
    )(first_blk, packed, packed, packed, packed, starts, cos_t, sin_t)


def assemble_kernel(turn, half_steps, rels, me_ref, *refs):
    out_ref = refs[-1]
    count = len(rels)

    def fill(ins):
        for rel, ref in zip(rels, ins):
            tokens = ref.shape[0]
            slot = me_ref[0] ^ rel
            if count == 2:
                slot = slot % 2
            place = pl.ds(pl.multiple_of(slot * tokens, tokens), tokens)
            if turn:
                out_ref[:, place] = ref[...].T
            else:
                out_ref[place, :] = ref[...]

    @pl.when(pl.program_id(0) < half_steps)
    def _():
        fill(refs[:count])

    @pl.when(pl.program_id(0) >= half_steps)
    def _():
        fill(refs[count:2 * count])


def assemble(got, rels, n_dev, prev, me, turn):
    low, high = [got[0][rel] for rel in rels], [got[1][rel] for rel in rels]
    tokens, half_width = low[0].shape
    seq, width = tokens * n_dev, 2 * half_width
    col_blk = 512
    steps = half_width // col_blk
    span = seq if prev is None else 2 * tokens
    pair = rels[0] // 2
    place = (lambda me: 0) if prev is None else (lambda me: (me[0] // 2) ^ pair)
    if turn:
        out_spec, shape = pl.BlockSpec((col_blk, span), lambda i, me: (i, place(me))), (width, seq)
    else:
        out_spec, shape = pl.BlockSpec((span, col_blk), lambda i, me: (place(me), i)), (seq, width)
    low_specs = [pl.BlockSpec((tokens, col_blk), lambda i, me: (0, jnp.minimum(i, steps - 1))) for _ in low]
    high_specs = [pl.BlockSpec((tokens, col_blk), lambda i, me: (0, jnp.maximum(i - steps, 0))) for _ in high]
    body = functools.partial(assemble_kernel, turn, steps, rels)
    extra, extra_specs, alias = [], [], {}
    if prev is not None:
        extra, extra_specs, alias = [prev], [pl.BlockSpec(memory_space=pl.ANY)], {1 + 2 * len(rels): 0}
    return pl.pallas_call(
        body,
        grid_spec=pltpu.PrefetchScalarGridSpec(
            num_scalar_prefetch=1,
            grid=(2 * steps,),
            in_specs=low_specs + high_specs + extra_specs,
            out_specs=out_spec,
        ),
        out_shape=jax.ShapeDtypeStruct(shape, BF16),
        input_output_aliases=alias,
        compiler_params=pltpu.CompilerParams(dimension_semantics=("arbitrary",), vmem_limit_bytes=60 * 1024 * 1024),
        cost_estimate=pl.CostEstimate(flops=0, bytes_accessed=4 * len(rels) * tokens * width, transcendentals=0),
    )(me, *low, *high, *extra)


def own_kernel(kinds, turned, me_ref, *refs):
    n_parts = sum(len(rows) * count for rows, count in kinds)
    parts, weights, (out_ref, scr) = refs[:n_parts], refs[n_parts:-2], refs[-2:]

    @pl.when(pl.program_id(0) == 0)
    def _():
        at = start = 0
        for rows, count in kinds:
            unit = sum(rows)
            for rel in range(count):
                block = jnp.concatenate([parts[at + j][...] for j in range(len(rows))], axis=0)
                at += len(rows)
                place = pl.ds(pl.multiple_of(start + (me_ref[0] ^ rel) * unit, HEAD_DIM), unit)
                scr[:, place] = block.T
            start += unit * count

    total = None
    start = 0
    for (rows, count), weight in zip(kinds, weights):
        width = sum(rows) * count
        dot = dot_nt if turned else dot_nn
        term = dot(scr[:, start:start + width], weight[...])
        total = term if total is None else total + term
        start += width
    out_ref[...] = total.astype(BF16)


def own_product(groups, weights, me, tokens, turned):
    kinds = tuple((tuple(part.shape[0] for part in pieces[0]), len(pieces)) for pieces in groups)
    flat = [part for pieces in groups for piece in pieces for part in piece]
    width = weights[0].shape[0] if turned else weights[0].shape[1]
    depth = sum(sum(rows) * count for rows, count in kinds)
    blk = 512
    if turned:
        weight_specs = [pl.BlockSpec((blk, weight.shape[1]), lambda i, me: (i, 0)) for weight in weights]
    else:
        weight_specs = [pl.BlockSpec((weight.shape[0], blk), lambda i, me: (0, i)) for weight in weights]
    return pl.pallas_call(
        functools.partial(own_kernel, kinds, turned),
        grid_spec=pltpu.PrefetchScalarGridSpec(
            num_scalar_prefetch=1,
            grid=(width // blk,),
            in_specs=[pl.BlockSpec((part.shape[0], tokens), lambda i, me: (0, me[0]), pipeline_mode=pl.Buffered(1)) for part in flat] + weight_specs,
            out_specs=pl.BlockSpec((tokens, blk), lambda i, me: (0, i)),
            scratch_shapes=[pltpu.VMEM((tokens, depth), BF16)],
        ),
        out_shape=jax.ShapeDtypeStruct((tokens, width), BF16),
        compiler_params=pltpu.CompilerParams(dimension_semantics=("arbitrary",), vmem_limit_bytes=60 * 1024 * 1024),
        cost_estimate=pl.CostEstimate(flops=2 * tokens * width * depth, bytes_accessed=2 * depth * (width + tokens), transcendentals=0),
    )(me, *flat, *weights)


def wgrad_kernel(by_rows, rels, n_out, me_ref, big_ref, *refs):
    n_in = len(refs) - 3 - n_out
    in_refs, out_refs = refs[:n_in - n_out], refs[n_in:n_in + n_out]
    cat, acc, sems = refs[-3:]
    step, n_steps = pl.program_id(0), pl.num_programs(0)
    slot = lax.rem(step, 2)
    blk = 512
    unit = cat.shape[0] // (len(rels) * n_out)

    def copies(at_step, at_slot):
        out = []
        wide = pl.ds(pl.multiple_of(at_step * blk, blk), blk)
        for o in range(n_out):
            for j, rel in enumerate(rels):
                part = pl.ds((o * len(rels) + j) * unit, unit)
                place = pl.ds(pl.multiple_of((me_ref[0] ^ rel) * unit, unit), unit)
                if by_rows:
                    src, dst = acc.at[at_slot, part, :], out_refs[o].at[place, wide]
                else:
                    src, dst = acc.at[at_slot, :, part], out_refs[o].at[wide, place]
                out.append(pltpu.make_async_copy(src, dst, sems.at[at_slot, o * len(rels) + j]))
        return out

    @pl.when(step == 0)
    def _():
        row = 0
        for ref in in_refs:
            cat[row:row + ref.shape[0], :] = ref[...]
            row += ref.shape[0]

    @pl.when(step >= 2)
    def _():
        for copy in copies(step - 2, slot):
            copy.wait()

    if by_rows:
        acc[slot] = dot_nn(cat[...], big_ref[...])
    else:
        acc[slot] = dot_nt(big_ref[...], cat[...])
    for copy in copies(step, slot):
        copy.start()

    @pl.when(step == n_steps - 1)
    def _():
        for copy in copies(step - 1, 1 - slot):
            copy.wait()
        for copy in copies(step, slot):
            copy.wait()


def weight_grad(big, parts, rels, me, prev, by_rows, n_out, n_dev):
    seq = big.shape[0] if by_rows else big.shape[1]
    width = big.shape[1] if by_rows else big.shape[0]
    rows = sum(part.shape[0] for part in parts)
    unit = rows // (len(rels) * n_out)
    cols = unit * n_dev
    blk = 512
    shape = (cols, width) if by_rows else (width, cols)
    big_spec = pl.BlockSpec((seq, blk), lambda i, me: (0, i)) if by_rows else pl.BlockSpec((blk, seq), lambda i, me: (i, 0))
    acc_shape = (2, rows, blk) if by_rows else (2, blk, rows)
    prev = [] if prev is None else list(prev)
    any_spec = pl.BlockSpec(memory_space=pl.ANY)
    n_fixed = 2 + len(parts)
    body = functools.partial(wgrad_kernel, by_rows, rels, n_out)
    if not prev:
        inner = body
        body = lambda me_ref, big_ref, *refs: inner(me_ref, big_ref, *refs[:len(parts)], *([None] * n_out), *refs[len(parts):])
    return pl.pallas_call(
        body,
        grid_spec=pltpu.PrefetchScalarGridSpec(
            num_scalar_prefetch=1,
            grid=(width // blk,),
            in_specs=[big_spec] + [pl.BlockSpec(part.shape, lambda i, me: (0, 0), pipeline_mode=pl.Buffered(1)) for part in parts] + [any_spec] * len(prev),
            out_specs=[any_spec] * n_out,
            scratch_shapes=[
                pltpu.VMEM((rows, seq), BF16),
                pltpu.VMEM(acc_shape, F32),
                pltpu.SemaphoreType.DMA((2, len(rels) * n_out)),
            ],
        ),
        out_shape=[jax.ShapeDtypeStruct(shape, F32)] * n_out,
        input_output_aliases={n_fixed + o: o for o in range(len(prev))},
        compiler_params=pltpu.CompilerParams(dimension_semantics=("arbitrary",), vmem_limit_bytes=60 * 1024 * 1024),
        cost_estimate=pl.CostEstimate(flops=2 * rows * width * seq, bytes_accessed=4 * width * rows + 2 * seq * (width + rows), transcendentals=0),
    )(me, big, *parts, *prev)


CORE, SIDE_X, SIDE_Y = 1, 2, 4


def solution(mesh):
    n_dev = mesh.shape["sp"]

    def swap(values, bit):
        return lax.ppermute(values, "sp", [(i, i ^ bit) for i in range(n_dev)])

    def reach(first, second):
        return tuple({0: own, SIDE_X: swap(own, SIDE_X), SIDE_Y: swap(own, SIDE_Y)} for own in (first, second))

    def relay(got):
        one, two = got
        one[SIDE_X | SIDE_Y] = swap(one[SIDE_Y], SIDE_X)
        two[SIDE_X | SIDE_Y] = swap(two[SIDE_X], SIDE_Y)
        for part in got:
            for rel in (0, SIDE_X, SIDE_Y):
                part[rel | CORE] = swap(part[rel], CORE)

    def finish(got, dep=None):
        for part in got:
            far = part[SIDE_X | SIDE_Y]
            part[SIDE_X | SIDE_Y | CORE] = swap(far if dep is None else after(far, dep), CORE)

    def after(value, dep):
        return lax.optimization_barrier((value, dep))[0]

    def hold(got, dep):
        for part in got:
            for rel in (SIDE_X, SIDE_Y):
                part[rel] = after(part[rel], dep)

    def device_body(hidden, grad_out, positions, doc_ids, w_q, w_k, w_v, w_o):
        tokens = hidden.shape[0]
        seq = tokens * n_dev
        group = w_q.shape[1] // w_k.shape[1]
        freqs = rope_freqs()
        me = lax.axis_index("sp").astype(jnp.int32)
        me_arr = me[None]
        idx_all = lax.all_gather(jnp.stack([positions, doc_ids])[None], "sp", axis=0, tiled=True)
        idx_all, hidden, grad_out = lax.optimization_barrier((idx_all, hidden, grad_out))
        pos_all = idx_all[:, 0, :].reshape(seq)
        doc_all = idx_all[:, 1, :].reshape(seq)
        starts = jnp.sum((doc_all[None, :] < doc_all[:, None]).astype(jnp.int32), axis=1)
        first_blk = starts[::BLK] // BLK

        angles = positions.astype(F32)[:, None] * freqs[None, :]
        cos_loc, sin_loc = jnp.cos(angles), jnp.sin(angles)
        cos_tab = jnp.concatenate([cos_loc, cos_loc], axis=1)
        sin_tab = jnp.concatenate([-sin_loc, sin_loc], axis=1)
        angles_t = freqs[:, None] * pos_all.astype(F32)[None, :]
        cos_t, sin_t = jnp.cos(angles_t), jnp.sin(angles_t)

        every = tuple(range(n_dev))
        groups = ((0, 1), (2, 3, 4, 5), (6, 7))

        def pairs(got, rels):
            return [half[r] for r in rels for half in got]

        half = hidden.shape[1] // 2
        x_got = reach(hidden[:, :half], hidden[:, half:])
        packed = project(hidden, grad_out, w_q, w_k, w_v, w_o, cos_tab, sin_tab, n_dev, group)
        packed = lax.all_to_all(packed, "sp", 0, 0, tiled=True).reshape(seq, -1)
        relay(x_got)
        near, far = tuple(range(6)), (6, 7)
        x_turned = assemble(x_got, near, n_dev, None, me_arr, True)
        g_got = reach(grad_out[:, :half], grad_out[:, half:])
        ctx_lo, ctx_hi, dq_lo, dq_hi, dk_t, dv_t = attention(packed, first_blk, starts[None, :], cos_t, sin_t, group)
        finish(x_got, dk_t)
        kv_got = reach(dk_t, dv_t)
        ctx_got = reach(ctx_lo, ctx_hi)
        dq_got = reach(dq_lo, dq_hi)

        x_turned = assemble(x_got, far, n_dev, x_turned, after(me_arr, dk_t), True)
        hold(g_got, x_turned)
        relay(g_got)
        (g_q,) = weight_grad(x_turned, pairs(dq_got, (0,)) + [swap(dq_got[0][0], CORE), swap(dq_got[1][0], CORE)], groups[0], me_arr, None, False, 1, n_dev)
        g_all = assemble(g_got, near, n_dev, None, after(me_arr, g_q), False)
        finish(g_got, g_all)
        g_all = assemble(g_got, far, n_dev, g_all, me_arr, False)
        (g_o,) = weight_grad(g_all, pairs(ctx_got, (0,)) + [swap(ctx_got[0][0], CORE), swap(ctx_got[1][0], CORE)], groups[0], me_arr, None, True, 1, n_dev)
        hold(ctx_got, g_o)
        relay(ctx_got)
        (g_o,) = weight_grad(g_all, pairs(ctx_got, groups[1]), groups[1], me_arr, (g_o,), True, 1, n_dev)
        finish(ctx_got, g_o)
        (g_o,) = weight_grad(g_all, pairs(ctx_got, groups[2]), groups[2], me_arr, (g_o,), True, 1, n_dev)
        hold(kv_got, g_o)
        relay(kv_got)
        attn_out = own_product([[[part[r] for part in ctx_got] for r in every]], [w_o], after(me_arr, g_o), tokens, False)
        finish(kv_got, attn_out)
        g_k, g_v = weight_grad(x_turned, [kv_got[0][r] for r in every] + [kv_got[1][r] for r in every], every, after(me_arr, attn_out), None, False, 2, n_dev)
        hold(dq_got, g_k)
        relay(dq_got)
        (g_q,) = weight_grad(x_turned, pairs(dq_got, groups[1]), groups[1], after(me_arr, g_k), (g_q,), False, 1, n_dev)
        finish(dq_got, g_q)
        (g_q,) = weight_grad(x_turned, pairs(dq_got, groups[2]), groups[2], me_arr, (g_q,), False, 1, n_dev)
        sources = [[[part[r] for part in dq_got] for r in every], [[kv_got[0][r]] for r in every], [[kv_got[1][r]] for r in every]]
        grad_hidden = own_product(sources, [w_q, w_k, w_v], after(me_arr, g_q), tokens, True)
        return attn_out, grad_hidden, g_q, g_k, g_v, g_o

    tok_spec = P(("dp", "sp"), None)
    vec_spec = P(("dp", "sp"))
    rep_spec = P(None, None)
    part_spec = P("dp", None)
    return jax.shard_map(device_body, mesh=mesh, in_specs=(tok_spec, tok_spec, vec_spec, vec_spec, rep_spec, rep_spec, rep_spec, rep_spec), out_specs=(tok_spec, tok_spec, part_spec, part_spec, part_spec, part_spec), check_vma=False)
```

```python
import functools
import math

import jax
import jax.numpy as jnp
from jax import lax
from jax.experimental import pallas as pl
from jax.experimental.pallas import tpu as pltpu
from jax.sharding import PartitionSpec as P


HEAD_DIM = 128
HALF = HEAD_DIM // 2
ROPE_THETA = 500000.0
ROPE_FACTOR = 8.0
ROPE_LOW = 1.0
ROPE_HIGH = 4.0
ROPE_OLD_CTX = 8192.0
NEG_BIG = -1.0e30
BLK = 256
F32 = jnp.float32
BF16 = jnp.bfloat16


def rope_freqs():
    half_idx = jnp.arange(HALF, dtype=F32)
    inv_freq = jnp.power(ROPE_THETA, -2.0 * half_idx / HEAD_DIM)
    wavelen = 2.0 * jnp.pi / inv_freq
    smooth = (ROPE_OLD_CTX / wavelen - ROPE_LOW) / (ROPE_HIGH - ROPE_LOW)
    mixed_freq = (1.0 - smooth) * inv_freq / ROPE_FACTOR + smooth * inv_freq
    scaled = jnp.where(wavelen > ROPE_OLD_CTX / ROPE_LOW, inv_freq / ROPE_FACTOR, mixed_freq)
    return jnp.where(wavelen < ROPE_OLD_CTX / ROPE_HIGH, inv_freq, scaled)


def dot_nn(lhs, rhs):
    return lax.dot_general(lhs, rhs, (((1,), (0,)), ((), ())), preferred_element_type=F32)


def dot_nt(lhs, rhs):
    return lax.dot_general(lhs, rhs, (((1,), (1,)), ((), ())), preferred_element_type=F32)


def proj_kernel(group, x_ref, g_ref, wq_ref, wk_ref, wv_ref, wo_ref, cos_ref, sin_ref, out_ref):
    cos_tab, sin_tab = cos_ref[...], sin_ref[...]

    def rope(val):
        return (val * cos_tab + pltpu.roll(val, HALF, 1) * sin_tab).astype(BF16)

    width = group * HEAD_DIM
    q_val = dot_nn(x_ref[...], wq_ref[...])
    for head in range(group):
        cols = slice(head * HEAD_DIM, (head + 1) * HEAD_DIM)
        out_ref[0, :, cols] = rope(q_val[:, cols])
    out_ref[0, :, width:2 * width] = dot_nt(g_ref[...], wo_ref[...]).astype(BF16)
    out_ref[0, :, 2 * width:2 * width + HEAD_DIM] = rope(dot_nn(x_ref[...], wk_ref[...]))
    out_ref[0, :, 2 * width + HEAD_DIM:] = dot_nn(x_ref[...], wv_ref[...]).astype(BF16)


def project(hidden, grad_out, w_q, w_k, w_v, w_o, cos_tab, sin_tab, n_dev, group):
    tokens, width = hidden.shape
    cols = group * HEAD_DIM
    total = 2 * cols + 2 * HEAD_DIM
    flops = 2 * tokens * width * n_dev * total
    return pl.pallas_call(
        functools.partial(proj_kernel, group),
        grid=(n_dev,),
        in_specs=[
            pl.BlockSpec((tokens, width), lambda i: (0, 0)),
            pl.BlockSpec((tokens, width), lambda i: (0, 0)),
            pl.BlockSpec((width, cols), lambda i: (0, i)),
            pl.BlockSpec((width, HEAD_DIM), lambda i: (0, i)),
            pl.BlockSpec((width, HEAD_DIM), lambda i: (0, i)),
            pl.BlockSpec((cols, width), lambda i: (i, 0)),
            pl.BlockSpec((tokens, HEAD_DIM), lambda i: (0, 0)),
            pl.BlockSpec((tokens, HEAD_DIM), lambda i: (0, 0)),
        ],
        out_specs=pl.BlockSpec((1, tokens, total), lambda i: (i, 0, 0)),
        out_shape=jax.ShapeDtypeStruct((n_dev, tokens, total), BF16),
        compiler_params=pltpu.CompilerParams(dimension_semantics=("arbitrary",), vmem_limit_bytes=60 * 1024 * 1024),
        cost_estimate=pl.CostEstimate(flops=flops, bytes_accessed=60_000_000, transcendentals=0),
        name="project",
    )(hidden, grad_out, w_q, w_k, w_v, w_o, cos_tab, sin_tab)


def attn_kernel(group, lo_ref, q_ref, do_ref, k_ref, v_ref, start_ref, cos_ref, sin_ref,
                ctx_lo, ctx_hi, dq_lo, dq_hi, dk_ref, dv_ref,
                s_scr, dp_scr, dk_acc, dv_acc, kt_scr, vt_scr, ctx_acc, dq_acc):
    blk = pl.program_id(0)
    n_blk = pl.num_programs(0)
    seq = k_ref.shape[0]
    scale = HEAD_DIM ** -0.5
    exp_scale = scale * math.log2(math.e)

    @pl.when(blk == 0)
    def _():
        dk_acc[...] = jnp.zeros_like(dk_acc)
        dv_acc[...] = jnp.zeros_like(dv_acc)

        @pl.loop(0, seq // BLK)
        def _(c):
            rows = pl.ds(pl.multiple_of(c * BLK, BLK), BLK)
            kt_scr[:, rows] = k_ref[rows, :].astype(F32).T.astype(BF16)
            vt_scr[:, rows] = v_ref[rows, :].astype(F32).T.astype(BF16)

    first = lo_ref[blk]
    last = blk + 1
    heads = [slice(h * HEAD_DIM, (h + 1) * HEAD_DIM) for h in range(group)]
    lanes = [slice(h * BLK, (h + 1) * BLK) for h in range(group)]
    starts = start_ref[...]
    q_idx = blk * BLK + lax.broadcasted_iota(jnp.int32, (1, BLK), 1)
    key_iota = lax.broadcasted_iota(jnp.int32, (BLK, BLK), 0)

    def score_step(c, peaks):
        rows = pl.ds(pl.multiple_of(c * BLK, BLK), BLK)
        key_idx = key_iota + c * BLK
        allowed = (key_idx >= starts) & (key_idx <= q_idx)
        k_blk = k_ref[rows, :]
        out = []
        for h in range(group):
            scores = jnp.where(allowed, dot_nt(k_blk, q_ref[:, heads[h]]), NEG_BIG)
            s_scr[rows, lanes[h]] = scores
            out.append(jnp.maximum(peaks[h], jnp.max(scores, axis=0, keepdims=True)))
        return tuple(out)

    peaks = lax.fori_loop(first, last, score_step, tuple(jnp.full((1, BLK), NEG_BIG, F32) for _ in range(group)))
    peaks = tuple(peak * exp_scale for peak in peaks)

    def exp_step(c, sums):
        rows = pl.ds(pl.multiple_of(c * BLK, BLK), BLK)
        v_blk = v_ref[rows, :]
        out = []
        for h in range(group):
            probs = jnp.exp2(s_scr[rows, lanes[h]] * exp_scale - peaks[h])
            d_prob = dot_nt(v_blk, do_ref[:, heads[h]])
            s_scr[rows, lanes[h]] = probs
            dp_scr[rows, lanes[h]] = d_prob
            out.append(sums[2 * h] + jnp.sum(probs, axis=0, keepdims=True))
            out.append(sums[2 * h + 1] + jnp.sum(probs * d_prob, axis=0, keepdims=True))
        return tuple(out)

    sums = lax.fori_loop(first, last, exp_step, tuple(jnp.zeros((1, BLK), F32) for _ in range(2 * group)))
    inv_sum = [1.0 / sums[2 * h] for h in range(group)]
    row_dot = [sums[2 * h + 1] * inv_sum[h] for h in range(group)]

    ctx_acc[...] = jnp.zeros_like(ctx_acc)
    dq_acc[...] = jnp.zeros_like(dq_acc)

    def grad_step(c, carry):
        rows = pl.ds(pl.multiple_of(c * BLK, BLK), BLK)
        k_t, v_t = kt_scr[:, rows], vt_scr[:, rows]
        dk_sum, dv_sum = dk_acc[rows, :], dv_acc[rows, :]
        for h in range(group):
            probs = s_scr[rows, lanes[h]] * inv_sum[h]
            probs_bf = probs.astype(BF16)
            d_score = (probs * (dp_scr[rows, lanes[h]] - row_dot[h]) * scale).astype(BF16)
            ctx_acc[:, lanes[h]] += dot_nn(v_t, probs_bf)
            dq_acc[:, lanes[h]] += dot_nn(k_t, d_score)
            dk_sum = dk_sum + dot_nn(d_score, q_ref[:, heads[h]])
            dv_sum = dv_sum + dot_nn(probs_bf, do_ref[:, heads[h]])
        dk_acc[rows, :] = dk_sum
        dv_acc[rows, :] = dv_sum
        return carry

    lax.fori_loop(first, last, grad_step, 0)

    def unrope(val, cos_tab, sin_tab):
        upper, lower = val[:HALF], val[HALF:]
        return (upper * cos_tab + lower * sin_tab).astype(BF16), (lower * cos_tab - upper * sin_tab).astype(BF16)

    own = pl.ds(pl.multiple_of(blk * BLK, BLK), BLK)
    cos_q, sin_q = cos_ref[:, own], sin_ref[:, own]
    half = ctx_lo.shape[0]
    for h in range(group):
        ctx_val = ctx_acc[:, lanes[h]].astype(BF16)
        dq_val = unrope(dq_acc[:, lanes[h]].astype(BF16).astype(F32), cos_q, sin_q)
        for part in range(2):
            row = h * HEAD_DIM + part * HALF
            ctx_out, dq_out = (ctx_lo, dq_lo) if row < half else (ctx_hi, dq_hi)
            place = slice(row % half, row % half + HALF)
            ctx_out[place, :] = ctx_val[part * HALF:(part + 1) * HALF]
            dq_out[place, :] = dq_val[part]

    @pl.when(blk == n_blk - 1)
    def _():
        @pl.loop(0, seq // BLK)
        def _(c):
            rows = pl.ds(pl.multiple_of(c * BLK, BLK), BLK)
            upper, lower = unrope(dk_acc[rows, :].T.astype(BF16).astype(F32), cos_ref[:, rows], sin_ref[:, rows])
            dk_ref[:HALF, rows] = upper
            dk_ref[HALF:, rows] = lower
            dv_ref[:, rows] = dv_acc[rows, :].T.astype(BF16)


def attention(packed, first_blk, starts, cos_t, sin_t, group):
    seq = packed.shape[0]
    cols = group * HEAD_DIM
    n_blk = seq // BLK
    grid_spec = pltpu.PrefetchScalarGridSpec(
        num_scalar_prefetch=1,
        grid=(n_blk,),
        in_specs=[
            pl.BlockSpec((BLK, cols), lambda i, lo: (i, 0)),
            pl.BlockSpec((BLK, cols), lambda i, lo: (i, 1)),
            pl.BlockSpec((seq, HEAD_DIM), lambda i, lo: (0, 2 * group)),
            pl.BlockSpec((seq, HEAD_DIM), lambda i, lo: (0, 2 * group + 1)),
            pl.BlockSpec((1, BLK), lambda i, lo: (0, i)),
            pl.BlockSpec((HALF, seq), lambda i, lo: (0, 0)),
            pl.BlockSpec((HALF, seq), lambda i, lo: (0, 0)),
        ],
        out_specs=[
            pl.BlockSpec((cols // 2, BLK), lambda i, lo: (0, i)),
            pl.BlockSpec((cols // 2, BLK), lambda i, lo: (0, i)),
            pl.BlockSpec((cols // 2, BLK), lambda i, lo: (0, i)),
            pl.BlockSpec((cols // 2, BLK), lambda i, lo: (0, i)),
            pl.BlockSpec((HEAD_DIM, seq), lambda i, lo: (0, 0)),
            pl.BlockSpec((HEAD_DIM, seq), lambda i, lo: (0, 0)),
        ],
        scratch_shapes=[
            pltpu.VMEM((seq, group * BLK), F32),
            pltpu.VMEM((seq, group * BLK), F32),
            pltpu.VMEM((seq, HEAD_DIM), F32),
            pltpu.VMEM((seq, HEAD_DIM), F32),
            pltpu.VMEM((HEAD_DIM, seq), BF16),
            pltpu.VMEM((HEAD_DIM, seq), BF16),
            pltpu.VMEM((HEAD_DIM, group * BLK), F32),
            pltpu.VMEM((HEAD_DIM, group * BLK), F32),
        ],
    )
    return pl.pallas_call(
        functools.partial(attn_kernel, group),
        grid_spec=grid_spec,
        out_shape=[
            jax.ShapeDtypeStruct((cols // 2, seq), BF16),
            jax.ShapeDtypeStruct((cols // 2, seq), BF16),
            jax.ShapeDtypeStruct((cols // 2, seq), BF16),
            jax.ShapeDtypeStruct((cols // 2, seq), BF16),
            jax.ShapeDtypeStruct((HEAD_DIM, seq), BF16),
            jax.ShapeDtypeStruct((HEAD_DIM, seq), BF16),
        ],
        compiler_params=pltpu.CompilerParams(dimension_semantics=("arbitrary",), vmem_limit_bytes=56 * 1024 * 1024),
        cost_estimate=pl.CostEstimate(flops=60 * seq * seq * HEAD_DIM, bytes_accessed=12_000_000, transcendentals=group * seq * seq // 2),
        name="attention",
    )(first_blk, packed, packed, packed, packed, starts, cos_t, sin_t)


def assemble_kernel(turn, half_steps, rels, me_ref, *refs):
    out_ref = refs[-1]
    count = len(rels)

    def fill(ins):
        for rel, ref in zip(rels, ins):
            tokens = ref.shape[0]
            slot = me_ref[0] ^ rel
            if count == 2:
                slot = slot % 2
            place = pl.ds(pl.multiple_of(slot * tokens, tokens), tokens)
            if turn:
                out_ref[:, place] = ref[...].T
            else:
                out_ref[place, :] = ref[...]

    @pl.when(pl.program_id(0) < half_steps)
    def _():
        fill(refs[:count])

    @pl.when(pl.program_id(0) >= half_steps)
    def _():
        fill(refs[count:2 * count])


def assemble(got, rels, n_dev, prev, me, turn):
    low, high = [got[0][rel] for rel in rels], [got[1][rel] for rel in rels]
    tokens, half_width = low[0].shape
    seq, width = tokens * n_dev, 2 * half_width
    col_blk = 512
    steps = half_width // col_blk
    span = seq if prev is None else 2 * tokens
    pair = rels[0] // 2
    place = (lambda me: 0) if prev is None else (lambda me: (me[0] // 2) ^ pair)
    if turn:
        out_spec, shape = pl.BlockSpec((col_blk, span), lambda i, me: (i, place(me))), (width, seq)
    else:
        out_spec, shape = pl.BlockSpec((span, col_blk), lambda i, me: (place(me), i)), (seq, width)
    low_specs = [pl.BlockSpec((tokens, col_blk), lambda i, me: (0, jnp.minimum(i, steps - 1))) for _ in low]
    high_specs = [pl.BlockSpec((tokens, col_blk), lambda i, me: (0, jnp.maximum(i - steps, 0))) for _ in high]
    body = functools.partial(assemble_kernel, turn, steps, rels)
    extra, extra_specs, alias = [], [], {}
    if prev is not None:
        extra, extra_specs, alias = [prev], [pl.BlockSpec(memory_space=pl.ANY)], {1 + 2 * len(rels): 0}
    return pl.pallas_call(
        body,
        grid_spec=pltpu.PrefetchScalarGridSpec(
            num_scalar_prefetch=1,
            grid=(2 * steps,),
            in_specs=low_specs + high_specs + extra_specs,
            out_specs=out_spec,
        ),
        out_shape=jax.ShapeDtypeStruct(shape, BF16),
        input_output_aliases=alias,
        compiler_params=pltpu.CompilerParams(dimension_semantics=("arbitrary",), vmem_limit_bytes=60 * 1024 * 1024),
        cost_estimate=pl.CostEstimate(flops=0, bytes_accessed=4 * len(rels) * tokens * width, transcendentals=0),
    )(me, *low, *high, *extra)


def own_kernel(kinds, turned, me_ref, *refs):
    n_parts = sum(len(rows) * count for rows, count in kinds)
    parts, weights, (out_ref, scr) = refs[:n_parts], refs[n_parts:-2], refs[-2:]

    @pl.when(pl.program_id(0) == 0)
    def _():
        at = start = 0
        for rows, count in kinds:
            unit = sum(rows)
            for rel in range(count):
                block = jnp.concatenate([parts[at + j][...] for j in range(len(rows))], axis=0)
                at += len(rows)
                place = pl.ds(pl.multiple_of(start + (me_ref[0] ^ rel) * unit, HEAD_DIM), unit)
                scr[:, place] = block.T
            start += unit * count

    total = None
    start = 0
    for (rows, count), weight in zip(kinds, weights):
        width = sum(rows) * count
        dot = dot_nt if turned else dot_nn
        term = dot(scr[:, start:start + width], weight[...])
        total = term if total is None else total + term
        start += width
    out_ref[...] = total.astype(BF16)


def own_product(groups, weights, me, tokens, turned):
    kinds = tuple((tuple(part.shape[0] for part in pieces[0]), len(pieces)) for pieces in groups)
    flat = [part for pieces in groups for piece in pieces for part in piece]
    width = weights[0].shape[0] if turned else weights[0].shape[1]
    depth = sum(sum(rows) * count for rows, count in kinds)
    blk = 512
    if turned:
        weight_specs = [pl.BlockSpec((blk, weight.shape[1]), lambda i, me: (i, 0)) for weight in weights]
    else:
        weight_specs = [pl.BlockSpec((weight.shape[0], blk), lambda i, me: (0, i)) for weight in weights]
    return pl.pallas_call(
        functools.partial(own_kernel, kinds, turned),
        grid_spec=pltpu.PrefetchScalarGridSpec(
            num_scalar_prefetch=1,
            grid=(width // blk,),
            in_specs=[pl.BlockSpec((part.shape[0], tokens), lambda i, me: (0, me[0]), pipeline_mode=pl.Buffered(1)) for part in flat] + weight_specs,
            out_specs=pl.BlockSpec((tokens, blk), lambda i, me: (0, i)),
            scratch_shapes=[pltpu.VMEM((tokens, depth), BF16)],
        ),
        out_shape=jax.ShapeDtypeStruct((tokens, width), BF16),
        compiler_params=pltpu.CompilerParams(dimension_semantics=("arbitrary",), vmem_limit_bytes=60 * 1024 * 1024),
        cost_estimate=pl.CostEstimate(flops=2 * tokens * width * depth, bytes_accessed=2 * depth * (width + tokens), transcendentals=0),
    )(me, *flat, *weights)


def wgrad_kernel(by_rows, spots, unit, n_out, n_big, half_steps, me_ref, *refs):
    n_part = len(spots)
    parts, bigs = refs[:n_part], refs[n_part:n_part + n_big]
    first_scratch = len(refs) - (4 if n_big == 1 else 6)
    scratch, out_refs = refs[first_scratch:], refs[first_scratch - n_out:first_scratch]
    cat, acc, part_sems, out_sems = scratch[:4]
    step, n_steps = pl.program_id(0), pl.num_programs(0)
    slot = lax.rem(step, 2)
    blk = acc.shape[1] if not by_rows else acc.shape[2]

    def out_copies(at_step, at_slot):
        out = []
        wide = pl.ds(pl.multiple_of(at_step * blk, blk), blk)
        row = 0
        for j, ((o, rel, off), part) in enumerate(zip(spots, parts)):
            height = part.shape[0]
            base = (me_ref[0] ^ rel) * unit
            if by_rows:
                place = pl.ds(pl.multiple_of(base + off, HALF), height)
                out.append(pltpu.make_async_copy(acc.at[at_slot, row:row + height, :], out_refs[o].at[place, wide], out_sems.at[at_slot, j]))
            elif off == 0:
                place = pl.ds(pl.multiple_of(base, HEAD_DIM), unit)
                out.append(pltpu.make_async_copy(acc.at[at_slot, :, row:row + unit], out_refs[o].at[wide, place], out_sems.at[at_slot, j]))
            row += height
        return out

    def part_copies():
        row, out = 0, []
        for j, part in enumerate(parts):
            out.append(pltpu.make_async_copy(part, cat.at[row:row + part.shape[0], :], part_sems.at[j]))
            row += part.shape[0]
        return out

    @pl.when(step == 0)
    def _():
        for copy in part_copies():
            copy.start()

    if n_big > 1:
        big_scr, big_sems = scratch[4:]
        n_dev = n_big // 2
        tokens = bigs[0].shape[0]

        def big_copies(ins, at_step, at_slot):
            wide = pl.ds(pl.multiple_of(lax.rem(at_step, half_steps) * blk, blk), blk)
            out = []
            for rel, ref in enumerate(ins):
                place = pl.ds(pl.multiple_of((me_ref[0] ^ rel) * tokens, tokens), tokens)
                out.append(pltpu.make_async_copy(ref.at[:, wide], big_scr.at[at_slot, place, :], big_sems.at[at_slot, rel]))
            return out

        def fetch(at_step, at_slot):
            @pl.when(at_step < half_steps)
            def _():
                for copy in big_copies(bigs[:n_dev], at_step, at_slot):
                    copy.start()

            @pl.when(at_step >= half_steps)
            def _():
                for copy in big_copies(bigs[n_dev:], at_step, at_slot):
                    copy.start()

        @pl.when(step == 0)
        def _():
            fetch(step, slot)

        @pl.when(step + 1 < n_steps)
        def _():
            fetch(step + 1, 1 - slot)

    @pl.when(step == 0)
    def _():
        for copy in part_copies():
            copy.wait()

    if n_big > 1:
        for copy in big_copies(bigs[:n_dev], step, slot):
            copy.wait()
        big = big_scr[slot]
    else:
        big = bigs[0][...]

    @pl.when(step >= 2)
    def _():
        for copy in out_copies(step - 2, slot):
            copy.wait()

    acc[slot] = dot_nn(cat[...], big) if by_rows else dot_nt(big, cat[...])
    for copy in out_copies(step, slot):
        copy.start()

    @pl.when(step == n_steps - 1)
    def _():
        for copy in out_copies(step - 1, 1 - slot):
            copy.wait()
        for copy in out_copies(step, slot):
            copy.wait()


def weight_grad(bigs, parts, spots, unit, me, prev, by_rows, n_out, n_dev):
    n_big = len(bigs)
    seq = parts[0].shape[1]
    rows = sum(part.shape[0] for part in parts)
    blk = 512
    any_spec = pl.BlockSpec(memory_space=pl.ANY)
    width = bigs[0].shape[0] if n_big == 1 else 2 * bigs[0].shape[1]
    cols = unit * n_dev
    shape = (cols, width) if by_rows else (width, cols)
    big_specs = [pl.BlockSpec((blk, seq), lambda i, me: (i, 0))] if n_big == 1 else [any_spec] * n_big
    prev = [] if prev is None else list(prev)
    scratch = [
        pltpu.VMEM((rows, seq), BF16),
        pltpu.VMEM((2, rows, blk) if by_rows else (2, blk, rows), F32),
        pltpu.SemaphoreType.DMA((len(parts),)),
        pltpu.SemaphoreType.DMA((2, len(parts))),
    ]
    if n_big > 1:
        scratch += [pltpu.VMEM((2, seq, blk), BF16), pltpu.SemaphoreType.DMA((2, n_dev))]
    body = functools.partial(wgrad_kernel, by_rows, spots, unit, n_out, n_big, width // blk // 2)
    n_lead = 1 + len(parts) + n_big

    return pl.pallas_call(
        body,
        grid_spec=pltpu.PrefetchScalarGridSpec(
            num_scalar_prefetch=1,
            grid=(width // blk,),
            in_specs=[any_spec] * len(parts) + big_specs + [any_spec] * len(prev),
            out_specs=[any_spec] * n_out,
            scratch_shapes=scratch,
        ),
        out_shape=[jax.ShapeDtypeStruct(shape, F32)] * n_out,
        input_output_aliases={n_lead + o: o for o in range(len(prev))},
        compiler_params=pltpu.CompilerParams(dimension_semantics=("arbitrary",), vmem_limit_bytes=60 * 1024 * 1024),
        cost_estimate=pl.CostEstimate(flops=2 * rows * width * seq, bytes_accessed=4 * width * rows + 2 * seq * (width + rows), transcendentals=0),
    )(me, *parts, *bigs, *prev)


CORE, SIDE_X, SIDE_Y = 1, 2, 4


def solution(mesh):
    n_dev = mesh.shape["sp"]

    def swap(values, bit):
        return lax.ppermute(values, "sp", [(i, i ^ bit) for i in range(n_dev)])

    def reach(first, second):
        return tuple({0: own, SIDE_X: swap(own, SIDE_X), SIDE_Y: swap(own, SIDE_Y)} for own in (first, second))

    def relay(got):
        one, two = got
        one[SIDE_X | SIDE_Y] = swap(one[SIDE_Y], SIDE_X)
        two[SIDE_X | SIDE_Y] = swap(two[SIDE_X], SIDE_Y)
        for part in got:
            for rel in (0, SIDE_X, SIDE_Y):
                if rel | CORE not in part:
                    part[rel | CORE] = swap(part[rel], CORE)

    def finish(got, dep=None):
        for part in got:
            far = part[SIDE_X | SIDE_Y]
            part[SIDE_X | SIDE_Y | CORE] = swap(far if dep is None else after(far, dep), CORE)

    def after(value, dep):
        return lax.optimization_barrier((value, dep))[0]

    def hold(got, dep):
        for part in got:
            for rel in (SIDE_X, SIDE_Y):
                part[rel] = after(part[rel], dep)

    def device_body(hidden, grad_out, positions, doc_ids, w_q, w_k, w_v, w_o):
        tokens = hidden.shape[0]
        seq = tokens * n_dev
        group = w_q.shape[1] // w_k.shape[1]
        freqs = rope_freqs()
        me = lax.axis_index("sp").astype(jnp.int32)
        me_arr = me[None]
        idx_all = lax.all_gather(jnp.stack([positions, doc_ids])[None], "sp", axis=0, tiled=True)
        idx_all, hidden, grad_out = lax.optimization_barrier((idx_all, hidden, grad_out))
        pos_all = idx_all[:, 0, :].reshape(seq)
        doc_all = idx_all[:, 1, :].reshape(seq)
        starts = jnp.sum((doc_all[None, :] < doc_all[:, None]).astype(jnp.int32), axis=1)
        first_blk = starts[::BLK] // BLK

        angles = positions.astype(F32)[:, None] * freqs[None, :]
        cos_loc, sin_loc = jnp.cos(angles), jnp.sin(angles)
        cos_tab = jnp.concatenate([cos_loc, cos_loc], axis=1)
        sin_tab = jnp.concatenate([-sin_loc, sin_loc], axis=1)
        angles_t = freqs[:, None] * pos_all.astype(F32)[None, :]
        cos_t, sin_t = jnp.cos(angles_t), jnp.sin(angles_t)

        every = tuple(range(n_dev))
        groups = ((0, 1), (2, 3, 4, 5), (6, 7))

        feats = group * HEAD_DIM

        def pairs(got, rels):
            return [part[r] for r in rels for part in got]

        def places(rels, parts=(0, 1)):
            return tuple((0, r, part * (feats // 2)) for r in rels for part in parts)

        half = hidden.shape[1] // 2
        x_got = reach(hidden[:, :half], hidden[:, half:])
        packed = project(hidden, grad_out, w_q, w_k, w_v, w_o, cos_tab, sin_tab, n_dev, group)
        packed = lax.all_to_all(packed, "sp", 0, 0, tiled=True).reshape(seq, -1)
        relay(x_got)
        near, far = tuple(range(6)), (6, 7)
        x_turned = assemble(x_got, near, n_dev, None, me_arr, True)
        g_got = reach(grad_out[:, :half], grad_out[:, half:])
        ctx_lo, ctx_hi, dq_lo, dq_hi, dk_t, dv_t = attention(packed, first_blk, starts[None, :], cos_t, sin_t, group)
        finish(x_got, dk_t)
        kv_got = reach(dk_t, dv_t)
        ctx_got = reach(ctx_lo, ctx_hi)
        dq_got = reach(dq_lo, dq_hi)

        x_turned = assemble(x_got, far, n_dev, x_turned, after(me_arr, dk_t), True)
        hold(g_got, x_turned)
        relay(g_got)
        (g_q,) = weight_grad([x_turned], pairs(dq_got, (0,)) + [swap(dq_got[0][0], CORE), swap(dq_got[1][0], CORE)], places(groups[0]), feats, me_arr, None, False, 1, n_dev)
        finish(g_got, g_q)
        g_all = [part[r] for part in g_got for r in every]
        (g_o,) = weight_grad(g_all, pairs(ctx_got, (0,)) + [swap(ctx_got[0][0], CORE), swap(ctx_got[1][0], CORE)], places(groups[0]), feats, after(me_arr, g_q), None, True, 1, n_dev)
        for rel in (SIDE_X, SIDE_Y):
            ctx_got[0][rel] = after(ctx_got[0][rel], g_o)
            ctx_got[0][rel | CORE] = swap(ctx_got[0][rel], CORE)
        (g_o,) = weight_grad(g_all, [ctx_got[0][r] for r in groups[1]], places(groups[1], (0,)), feats, me_arr, (g_o,), True, 1, n_dev)
        for rel in (SIDE_X, SIDE_Y):
            ctx_got[1][rel] = after(ctx_got[1][rel], g_o)
        relay(ctx_got)
        (g_o,) = weight_grad(g_all, [ctx_got[1][r] for r in groups[1]], places(groups[1], (1,)), feats, me_arr, (g_o,), True, 1, n_dev)
        finish(ctx_got, g_o)
        (g_o,) = weight_grad(g_all, pairs(ctx_got, groups[2]), places(groups[2]), feats, me_arr, (g_o,), True, 1, n_dev)
        hold(kv_got, g_o)
        relay(kv_got)
        attn_out = own_product([[[part[r] for part in ctx_got] for r in every]], [w_o], after(me_arr, g_o), tokens, False)
        finish(kv_got, attn_out)
        kv_places = tuple((o, r, 0) for o in range(2) for r in every)
        g_k, g_v = weight_grad([x_turned], [kv_got[0][r] for r in every] + [kv_got[1][r] for r in every], kv_places, HEAD_DIM, after(me_arr, attn_out), None, False, 2, n_dev)
        hold(dq_got, g_k)
        relay(dq_got)
        (g_q,) = weight_grad([x_turned], pairs(dq_got, groups[1]), places(groups[1]), feats, after(me_arr, g_k), (g_q,), False, 1, n_dev)
        finish(dq_got, g_q)
        (g_q,) = weight_grad([x_turned], pairs(dq_got, groups[2]), places(groups[2]), feats, me_arr, (g_q,), False, 1, n_dev)
        sources = [[[part[r] for part in dq_got] for r in every], [[kv_got[0][r]] for r in every], [[kv_got[1][r]] for r in every]]
        grad_hidden = own_product(sources, [w_q, w_k, w_v], after(me_arr, g_q), tokens, True)
        return attn_out, grad_hidden, g_q, g_k, g_v, g_o

    tok_spec = P(("dp", "sp"), None)
    vec_spec = P(("dp", "sp"))
    rep_spec = P(None, None)
    part_spec = P("dp", None)
    return jax.shard_map(device_body, mesh=mesh, in_specs=(tok_spec, tok_spec, vec_spec, vec_spec, rep_spec, rep_spec, rep_spec, rep_spec), out_specs=(tok_spec, tok_spec, part_spec, part_spec, part_spec, part_spec), check_vma=False)
```

```python
import functools
import math

import jax
import jax.numpy as jnp
from jax import lax
from jax.experimental import pallas as pl
from jax.experimental.pallas import tpu as pltpu
from jax.sharding import PartitionSpec as P


HEAD_DIM = 128
HALF = HEAD_DIM // 2
ROPE_THETA = 500000.0
ROPE_FACTOR = 8.0
ROPE_LOW = 1.0
ROPE_HIGH = 4.0
ROPE_OLD_CTX = 8192.0
NEG_BIG = -1.0e30
BLK = 256
F32 = jnp.float32
BF16 = jnp.bfloat16


def rope_freqs():
    half_idx = jnp.arange(HALF, dtype=F32)
    inv_freq = jnp.power(ROPE_THETA, -2.0 * half_idx / HEAD_DIM)
    wavelen = 2.0 * jnp.pi / inv_freq
    smooth = (ROPE_OLD_CTX / wavelen - ROPE_LOW) / (ROPE_HIGH - ROPE_LOW)
    mixed_freq = (1.0 - smooth) * inv_freq / ROPE_FACTOR + smooth * inv_freq
    scaled = jnp.where(wavelen > ROPE_OLD_CTX / ROPE_LOW, inv_freq / ROPE_FACTOR, mixed_freq)
    return jnp.where(wavelen < ROPE_OLD_CTX / ROPE_HIGH, inv_freq, scaled)


def dot_nn(lhs, rhs):
    return lax.dot_general(lhs, rhs, (((1,), (0,)), ((), ())), preferred_element_type=F32)


def dot_nt(lhs, rhs):
    return lax.dot_general(lhs, rhs, (((1,), (1,)), ((), ())), preferred_element_type=F32)


def proj_kernel(group, x_ref, g_ref, wq_ref, wk_ref, wv_ref, wo_ref, cos_ref, sin_ref, out_ref):
    cos_tab, sin_tab = cos_ref[...], sin_ref[...]

    def rope(val):
        return (val * cos_tab + pltpu.roll(val, HALF, 1) * sin_tab).astype(BF16)

    width = group * HEAD_DIM
    q_val = dot_nn(x_ref[...], wq_ref[...])
    for head in range(group):
        cols = slice(head * HEAD_DIM, (head + 1) * HEAD_DIM)
        out_ref[0, :, cols] = rope(q_val[:, cols])
    out_ref[0, :, width:2 * width] = dot_nt(g_ref[...], wo_ref[...]).astype(BF16)
    out_ref[0, :, 2 * width:2 * width + HEAD_DIM] = rope(dot_nn(x_ref[...], wk_ref[...]))
    out_ref[0, :, 2 * width + HEAD_DIM:] = dot_nn(x_ref[...], wv_ref[...]).astype(BF16)


def project(hidden, grad_out, w_q, w_k, w_v, w_o, cos_tab, sin_tab, n_dev, group):
    tokens, width = hidden.shape
    cols = group * HEAD_DIM
    total = 2 * cols + 2 * HEAD_DIM
    flops = 2 * tokens * width * n_dev * total
    return pl.pallas_call(
        functools.partial(proj_kernel, group),
        grid=(n_dev,),
        in_specs=[
            pl.BlockSpec((tokens, width), lambda i: (0, 0)),
            pl.BlockSpec((tokens, width), lambda i: (0, 0)),
            pl.BlockSpec((width, cols), lambda i: (0, i)),
            pl.BlockSpec((width, HEAD_DIM), lambda i: (0, i)),
            pl.BlockSpec((width, HEAD_DIM), lambda i: (0, i)),
            pl.BlockSpec((cols, width), lambda i: (i, 0)),
            pl.BlockSpec((tokens, HEAD_DIM), lambda i: (0, 0)),
            pl.BlockSpec((tokens, HEAD_DIM), lambda i: (0, 0)),
        ],
        out_specs=pl.BlockSpec((1, tokens, total), lambda i: (i, 0, 0)),
        out_shape=jax.ShapeDtypeStruct((n_dev, tokens, total), BF16),
        compiler_params=pltpu.CompilerParams(dimension_semantics=("arbitrary",), vmem_limit_bytes=60 * 1024 * 1024),
        cost_estimate=pl.CostEstimate(flops=flops, bytes_accessed=60_000_000, transcendentals=0),
        name="project",
    )(hidden, grad_out, w_q, w_k, w_v, w_o, cos_tab, sin_tab)


def attn_kernel(group, lo_ref, q_ref, do_ref, k_ref, v_ref, start_ref, cos_ref, sin_ref,
                ctx_lo, ctx_hi, dq_lo, dq_hi, dk_ref, dv_ref,
                s_scr, dp_scr, dk_acc, dv_acc, kt_scr, vt_scr, ctx_acc, dq_acc):
    blk = pl.program_id(0)
    n_blk = pl.num_programs(0)
    seq = k_ref.shape[0]
    scale = HEAD_DIM ** -0.5
    exp_scale = scale * math.log2(math.e)

    @pl.when(blk == 0)
    def _():
        dk_acc[...] = jnp.zeros_like(dk_acc)
        dv_acc[...] = jnp.zeros_like(dv_acc)

        @pl.loop(0, seq // BLK)
        def _(c):
            rows = pl.ds(pl.multiple_of(c * BLK, BLK), BLK)
            kt_scr[:, rows] = k_ref[rows, :].astype(F32).T.astype(BF16)
            vt_scr[:, rows] = v_ref[rows, :].astype(F32).T.astype(BF16)

    first = lo_ref[blk]
    last = blk + 1
    heads = [slice(h * HEAD_DIM, (h + 1) * HEAD_DIM) for h in range(group)]
    lanes = [slice(h * BLK, (h + 1) * BLK) for h in range(group)]
    starts = start_ref[...]
    q_idx = blk * BLK + lax.broadcasted_iota(jnp.int32, (1, BLK), 1)
    key_iota = lax.broadcasted_iota(jnp.int32, (BLK, BLK), 0)

    def score_step(c, peaks):
        rows = pl.ds(pl.multiple_of(c * BLK, BLK), BLK)
        key_idx = key_iota + c * BLK
        allowed = (key_idx >= starts) & (key_idx <= q_idx)
        k_blk = k_ref[rows, :]
        out = []
        for h in range(group):
            scores = jnp.where(allowed, dot_nt(k_blk, q_ref[:, heads[h]]), NEG_BIG)
            s_scr[rows, lanes[h]] = scores
            out.append(jnp.maximum(peaks[h], jnp.max(scores, axis=0, keepdims=True)))
        return tuple(out)

    peaks = lax.fori_loop(first, last, score_step, tuple(jnp.full((1, BLK), NEG_BIG, F32) for _ in range(group)))
    peaks = tuple(peak * exp_scale for peak in peaks)

    def exp_step(c, sums):
        rows = pl.ds(pl.multiple_of(c * BLK, BLK), BLK)
        v_blk = v_ref[rows, :]
        out = []
        for h in range(group):
            probs = jnp.exp2(s_scr[rows, lanes[h]] * exp_scale - peaks[h])
            d_prob = dot_nt(v_blk, do_ref[:, heads[h]])
            s_scr[rows, lanes[h]] = probs
            dp_scr[rows, lanes[h]] = d_prob
            out.append(sums[2 * h] + jnp.sum(probs, axis=0, keepdims=True))
            out.append(sums[2 * h + 1] + jnp.sum(probs * d_prob, axis=0, keepdims=True))
        return tuple(out)

    sums = lax.fori_loop(first, last, exp_step, tuple(jnp.zeros((1, BLK), F32) for _ in range(2 * group)))
    inv_sum = [1.0 / sums[2 * h] for h in range(group)]
    row_dot = [sums[2 * h + 1] * inv_sum[h] for h in range(group)]

    ctx_acc[...] = jnp.zeros_like(ctx_acc)
    dq_acc[...] = jnp.zeros_like(dq_acc)

    def grad_step(c, carry):
        rows = pl.ds(pl.multiple_of(c * BLK, BLK), BLK)
        k_t, v_t = kt_scr[:, rows], vt_scr[:, rows]
        dk_sum, dv_sum = dk_acc[rows, :], dv_acc[rows, :]
        for h in range(group):
            probs = s_scr[rows, lanes[h]] * inv_sum[h]
            probs_bf = probs.astype(BF16)
            d_score = (probs * (dp_scr[rows, lanes[h]] - row_dot[h]) * scale).astype(BF16)
            ctx_acc[:, lanes[h]] += dot_nn(v_t, probs_bf)
            dq_acc[:, lanes[h]] += dot_nn(k_t, d_score)
            dk_sum = dk_sum + dot_nn(d_score, q_ref[:, heads[h]])
            dv_sum = dv_sum + dot_nn(probs_bf, do_ref[:, heads[h]])
        dk_acc[rows, :] = dk_sum
        dv_acc[rows, :] = dv_sum
        return carry

    lax.fori_loop(first, last, grad_step, 0)

    def unrope(val, cos_tab, sin_tab):
        upper, lower = val[:HALF], val[HALF:]
        return (upper * cos_tab + lower * sin_tab).astype(BF16), (lower * cos_tab - upper * sin_tab).astype(BF16)

    own = pl.ds(pl.multiple_of(blk * BLK, BLK), BLK)
    cos_q, sin_q = cos_ref[:, own], sin_ref[:, own]
    half = ctx_lo.shape[0]
    for h in range(group):
        ctx_val = ctx_acc[:, lanes[h]].astype(BF16)
        dq_val = unrope(dq_acc[:, lanes[h]].astype(BF16).astype(F32), cos_q, sin_q)
        for part in range(2):
            row = h * HEAD_DIM + part * HALF
            ctx_out, dq_out = (ctx_lo, dq_lo) if row < half else (ctx_hi, dq_hi)
            place = slice(row % half, row % half + HALF)
            ctx_out[place, :] = ctx_val[part * HALF:(part + 1) * HALF]
            dq_out[place, :] = dq_val[part]

    @pl.when(blk == n_blk - 1)
    def _():
        @pl.loop(0, seq // BLK)
        def _(c):
            rows = pl.ds(pl.multiple_of(c * BLK, BLK), BLK)
            upper, lower = unrope(dk_acc[rows, :].T.astype(BF16).astype(F32), cos_ref[:, rows], sin_ref[:, rows])
            dk_ref[:HALF, rows] = upper
            dk_ref[HALF:, rows] = lower
            dv_ref[:, rows] = dv_acc[rows, :].T.astype(BF16)


def attention(packed, first_blk, starts, cos_t, sin_t, group):
    seq = packed.shape[0]
    cols = group * HEAD_DIM
    n_blk = seq // BLK
    grid_spec = pltpu.PrefetchScalarGridSpec(
        num_scalar_prefetch=1,
        grid=(n_blk,),
        in_specs=[
            pl.BlockSpec((BLK, cols), lambda i, lo: (i, 0)),
            pl.BlockSpec((BLK, cols), lambda i, lo: (i, 1)),
            pl.BlockSpec((seq, HEAD_DIM), lambda i, lo: (0, 2 * group)),
            pl.BlockSpec((seq, HEAD_DIM), lambda i, lo: (0, 2 * group + 1)),
            pl.BlockSpec((1, BLK), lambda i, lo: (0, i)),
            pl.BlockSpec((HALF, seq), lambda i, lo: (0, 0)),
            pl.BlockSpec((HALF, seq), lambda i, lo: (0, 0)),
        ],
        out_specs=[
            pl.BlockSpec((cols // 2, BLK), lambda i, lo: (0, i)),
            pl.BlockSpec((cols // 2, BLK), lambda i, lo: (0, i)),
            pl.BlockSpec((cols // 2, BLK), lambda i, lo: (0, i)),
            pl.BlockSpec((cols // 2, BLK), lambda i, lo: (0, i)),
            pl.BlockSpec((HEAD_DIM, seq), lambda i, lo: (0, 0)),
            pl.BlockSpec((HEAD_DIM, seq), lambda i, lo: (0, 0)),
        ],
        scratch_shapes=[
            pltpu.VMEM((seq, group * BLK), F32),
            pltpu.VMEM((seq, group * BLK), F32),
            pltpu.VMEM((seq, HEAD_DIM), F32),
            pltpu.VMEM((seq, HEAD_DIM), F32),
            pltpu.VMEM((HEAD_DIM, seq), BF16),
            pltpu.VMEM((HEAD_DIM, seq), BF16),
            pltpu.VMEM((HEAD_DIM, group * BLK), F32),
            pltpu.VMEM((HEAD_DIM, group * BLK), F32),
        ],
    )
    return pl.pallas_call(
        functools.partial(attn_kernel, group),
        grid_spec=grid_spec,
        out_shape=[
            jax.ShapeDtypeStruct((cols // 2, seq), BF16),
            jax.ShapeDtypeStruct((cols // 2, seq), BF16),
            jax.ShapeDtypeStruct((cols // 2, seq), BF16),
            jax.ShapeDtypeStruct((cols // 2, seq), BF16),
            jax.ShapeDtypeStruct((HEAD_DIM, seq), BF16),
            jax.ShapeDtypeStruct((HEAD_DIM, seq), BF16),
        ],
        compiler_params=pltpu.CompilerParams(dimension_semantics=("arbitrary",), vmem_limit_bytes=56 * 1024 * 1024),
        cost_estimate=pl.CostEstimate(flops=60 * seq * seq * HEAD_DIM, bytes_accessed=12_000_000, transcendentals=group * seq * seq // 2),
        name="attention",
    )(first_blk, packed, packed, packed, packed, starts, cos_t, sin_t)


def assemble_kernel(turn, half_steps, rels, me_ref, *refs):
    out_ref = refs[-1]
    count = len(rels)

    def fill(ins):
        for rel, ref in zip(rels, ins):
            tokens = ref.shape[0]
            slot = me_ref[0] ^ rel
            if count == 2:
                slot = slot % 2
            place = pl.ds(pl.multiple_of(slot * tokens, tokens), tokens)
            if turn:
                out_ref[:, place] = ref[...].T
            else:
                out_ref[place, :] = ref[...]

    @pl.when(pl.program_id(0) < half_steps)
    def _():
        fill(refs[:count])

    @pl.when(pl.program_id(0) >= half_steps)
    def _():
        fill(refs[count:2 * count])


def assemble(got, rels, n_dev, prev, me, turn):
    low, high = [got[0][rel] for rel in rels], [got[1][rel] for rel in rels]
    tokens, half_width = low[0].shape
    seq, width = tokens * n_dev, 2 * half_width
    col_blk = 512
    steps = half_width // col_blk
    span = seq if prev is None else 2 * tokens
    pair = rels[0] // 2
    place = (lambda me: 0) if prev is None else (lambda me: (me[0] // 2) ^ pair)
    if turn:
        out_spec, shape = pl.BlockSpec((col_blk, span), lambda i, me: (i, place(me))), (width, seq)
    else:
        out_spec, shape = pl.BlockSpec((span, col_blk), lambda i, me: (place(me), i)), (seq, width)
    low_specs = [pl.BlockSpec((tokens, col_blk), lambda i, me: (0, jnp.minimum(i, steps - 1))) for _ in low]
    high_specs = [pl.BlockSpec((tokens, col_blk), lambda i, me: (0, jnp.maximum(i - steps, 0))) for _ in high]
    body = functools.partial(assemble_kernel, turn, steps, rels)
    extra, extra_specs, alias = [], [], {}
    if prev is not None:
        extra, extra_specs, alias = [prev], [pl.BlockSpec(memory_space=pl.ANY)], {1 + 2 * len(rels): 0}
    return pl.pallas_call(
        body,
        grid_spec=pltpu.PrefetchScalarGridSpec(
            num_scalar_prefetch=1,
            grid=(2 * steps,),
            in_specs=low_specs + high_specs + extra_specs,
            out_specs=out_spec,
        ),
        out_shape=jax.ShapeDtypeStruct(shape, BF16),
        input_output_aliases=alias,
        compiler_params=pltpu.CompilerParams(dimension_semantics=("arbitrary",), vmem_limit_bytes=60 * 1024 * 1024),
        cost_estimate=pl.CostEstimate(flops=0, bytes_accessed=4 * len(rels) * tokens * width, transcendentals=0),
    )(me, *low, *high, *extra)


def own_kernel(kinds, turned, me_ref, *refs):
    n_parts = sum(len(rows) * count for rows, count in kinds)
    parts, weights, (out_ref, scr) = refs[:n_parts], refs[n_parts:-2], refs[-2:]

    @pl.when(pl.program_id(0) == 0)
    def _():
        at = start = 0
        for rows, count in kinds:
            unit = sum(rows)
            for rel in range(count):
                block = jnp.concatenate([parts[at + j][...] for j in range(len(rows))], axis=0)
                at += len(rows)
                place = pl.ds(pl.multiple_of(start + (me_ref[0] ^ rel) * unit, HEAD_DIM), unit)
                scr[:, place] = block.T
            start += unit * count

    total = None
    start = 0
    for (rows, count), weight in zip(kinds, weights):
        width = sum(rows) * count
        dot = dot_nt if turned else dot_nn
        term = dot(scr[:, start:start + width], weight[...])
        total = term if total is None else total + term
        start += width
    out_ref[...] = total.astype(BF16)


def own_product(groups, weights, me, tokens, turned):
    kinds = tuple((tuple(part.shape[0] for part in pieces[0]), len(pieces)) for pieces in groups)
    flat = [part for pieces in groups for piece in pieces for part in piece]
    width = weights[0].shape[0] if turned else weights[0].shape[1]
    depth = sum(sum(rows) * count for rows, count in kinds)
    blk = 512
    if turned:
        weight_specs = [pl.BlockSpec((blk, weight.shape[1]), lambda i, me: (i, 0)) for weight in weights]
    else:
        weight_specs = [pl.BlockSpec((weight.shape[0], blk), lambda i, me: (0, i)) for weight in weights]
    return pl.pallas_call(
        functools.partial(own_kernel, kinds, turned),
        grid_spec=pltpu.PrefetchScalarGridSpec(
            num_scalar_prefetch=1,
            grid=(width // blk,),
            in_specs=[pl.BlockSpec((part.shape[0], tokens), lambda i, me: (0, me[0]), pipeline_mode=pl.Buffered(1)) for part in flat] + weight_specs,
            out_specs=pl.BlockSpec((tokens, blk), lambda i, me: (0, i)),
            scratch_shapes=[pltpu.VMEM((tokens, depth), BF16)],
        ),
        out_shape=jax.ShapeDtypeStruct((tokens, width), BF16),
        compiler_params=pltpu.CompilerParams(dimension_semantics=("arbitrary",), vmem_limit_bytes=60 * 1024 * 1024),
        cost_estimate=pl.CostEstimate(flops=2 * tokens * width * depth, bytes_accessed=2 * depth * (width + tokens), transcendentals=0),
    )(me, *flat, *weights)


def wgrad_kernel(by_rows, spots, unit, n_out, n_big, half_steps, me_ref, *refs):
    n_part = len(spots)
    parts, bigs = refs[:n_part], refs[n_part:n_part + n_big]
    first_scratch = len(refs) - 6
    scratch, out_refs = refs[first_scratch:], refs[first_scratch - n_out:first_scratch]
    cat, acc, part_sems, out_sems = scratch[:4]
    step, n_steps = pl.program_id(0), pl.num_programs(0)
    slot = lax.rem(step, 2)
    blk = acc.shape[1] if not by_rows else acc.shape[2]

    def out_copies(at_step, at_slot):
        out = []
        wide = pl.ds(pl.multiple_of(at_step * blk, blk), blk)
        row = 0
        for j, ((o, rel, off), part) in enumerate(zip(spots, parts)):
            height = part.shape[0]
            base = (me_ref[0] ^ rel) * unit
            if by_rows:
                place = pl.ds(pl.multiple_of(base + off, HALF), height)
                out.append(pltpu.make_async_copy(acc.at[at_slot, row:row + height, :], out_refs[o].at[place, wide], out_sems.at[at_slot, j]))
            elif off == 0:
                place = pl.ds(pl.multiple_of(base, HEAD_DIM), unit)
                out.append(pltpu.make_async_copy(acc.at[at_slot, :, row:row + unit], out_refs[o].at[wide, place], out_sems.at[at_slot, j]))
            row += height
        return out

    def part_copies():
        row, out = 0, []
        for j, part in enumerate(parts):
            out.append(pltpu.make_async_copy(part, cat.at[row:row + part.shape[0], :], part_sems.at[j]))
            row += part.shape[0]
        return out

    big_scr, big_sems = scratch[4:]
    n_dev = max(1, n_big // 2)

    def big_copies(ins, at_step, at_slot):
        if n_big == 1:
            deep = pl.ds(pl.multiple_of(at_step * blk, blk), blk)
            return [pltpu.make_async_copy(bigs[0].at[deep, :], big_scr.at[at_slot], big_sems.at[at_slot, 0])]
        tokens = bigs[0].shape[0]
        wide = pl.ds(pl.multiple_of(lax.rem(at_step, half_steps) * blk, blk), blk)
        out = []
        for rel, ref in enumerate(ins):
            place = pl.ds(pl.multiple_of((me_ref[0] ^ rel) * tokens, tokens), tokens)
            out.append(pltpu.make_async_copy(ref.at[:, wide], big_scr.at[at_slot, place, :], big_sems.at[at_slot, rel]))
        return out

    def fetch(at_step, at_slot):
        @pl.when(at_step < half_steps)
        def _():
            for copy in big_copies(bigs[:n_dev], at_step, at_slot):
                copy.start()

        @pl.when(at_step >= half_steps)
        def _():
            for copy in big_copies(bigs[-n_dev:], at_step, at_slot):
                copy.start()

    @pl.when(step == 0)
    def _():
        fetch(step, slot)
        for copy in part_copies():
            copy.start()

    @pl.when(step + 1 < n_steps)
    def _():
        fetch(step + 1, 1 - slot)

    for copy in big_copies(bigs[:n_dev], step, slot):
        copy.wait()

    @pl.when(step >= 2)
    def _():
        for copy in out_copies(step - 2, slot):
            copy.wait()

    limit = 384 if by_rows else 768
    at, row = 0, 0
    while at < n_part:
        until, height = at, 0
        while until < n_part and height + parts[until].shape[0] <= limit:
            height += parts[until].shape[0]
            until += 1

        @pl.when(step == 0)
        def _(at=at, until=until):
            for copy in part_copies()[at:until]:
                copy.wait()

        if by_rows:
            acc[slot, row:row + height, :] = dot_nn(cat[row:row + height, :], big_scr[slot])
        else:
            acc[slot, :, row:row + height] = dot_nt(big_scr[slot], cat[row:row + height, :])
        at, row = until, row + height

    for copy in out_copies(step, slot):
        copy.start()

    @pl.when(step == n_steps - 1)
    def _():
        for copy in out_copies(step - 1, 1 - slot):
            copy.wait()
        for copy in out_copies(step, slot):
            copy.wait()


def weight_grad(bigs, parts, spots, unit, me, prev, by_rows, n_out, n_dev):
    n_big = len(bigs)
    seq = parts[0].shape[1]
    rows = sum(part.shape[0] for part in parts)
    blk = 512
    any_spec = pl.BlockSpec(memory_space=pl.ANY)
    width = bigs[0].shape[0] if n_big == 1 else 2 * bigs[0].shape[1]
    cols = unit * n_dev
    shape = (cols, width) if by_rows else (width, cols)
    big_specs = [any_spec] * n_big
    prev = [] if prev is None else list(prev)
    scratch = [
        pltpu.VMEM((rows, seq), BF16),
        pltpu.VMEM((2, rows, blk) if by_rows else (2, blk, rows), F32),
        pltpu.SemaphoreType.DMA((len(parts),)),
        pltpu.SemaphoreType.DMA((2, len(parts))),
    ]
    scratch += [pltpu.VMEM((2, seq, blk) if by_rows else (2, blk, seq), BF16), pltpu.SemaphoreType.DMA((2, n_dev))]
    body = functools.partial(wgrad_kernel, by_rows, spots, unit, n_out, n_big, width // blk // 2)
    n_lead = 1 + len(parts) + n_big

    return pl.pallas_call(
        body,
        grid_spec=pltpu.PrefetchScalarGridSpec(
            num_scalar_prefetch=1,
            grid=(width // blk,),
            in_specs=[any_spec] * len(parts) + big_specs + [any_spec] * len(prev),
            out_specs=[any_spec] * n_out,
            scratch_shapes=scratch,
        ),
        out_shape=[jax.ShapeDtypeStruct(shape, F32)] * n_out,
        input_output_aliases={n_lead + o: o for o in range(len(prev))},
        compiler_params=pltpu.CompilerParams(dimension_semantics=("arbitrary",), vmem_limit_bytes=60 * 1024 * 1024),
        cost_estimate=pl.CostEstimate(flops=2 * rows * width * seq, bytes_accessed=4 * width * rows + 2 * seq * (width + rows), transcendentals=0),
    )(me, *parts, *bigs, *prev)


CORE, SIDE_X, SIDE_Y = 1, 2, 4


def solution(mesh):
    n_dev = mesh.shape["sp"]

    def swap(values, bit):
        return lax.ppermute(values, "sp", [(i, i ^ bit) for i in range(n_dev)])

    def reach(first, second):
        return tuple({0: own, SIDE_X: swap(own, SIDE_X), SIDE_Y: swap(own, SIDE_Y)} for own in (first, second))

    def relay(got):
        one, two = got
        one[SIDE_X | SIDE_Y] = swap(one[SIDE_Y], SIDE_X)
        two[SIDE_X | SIDE_Y] = swap(two[SIDE_X], SIDE_Y)
        for part in got:
            for rel in (0, SIDE_X, SIDE_Y):
                if rel | CORE not in part:
                    part[rel | CORE] = swap(part[rel], CORE)

    def finish(got, dep=None):
        for part in got:
            far = part[SIDE_X | SIDE_Y]
            part[SIDE_X | SIDE_Y | CORE] = swap(far if dep is None else after(far, dep), CORE)

    def after(value, dep):
        return lax.optimization_barrier((value, dep))[0]

    def hold(got, dep):
        for part in got:
            for rel in (SIDE_X, SIDE_Y):
                part[rel] = after(part[rel], dep)

    def device_body(hidden, grad_out, positions, doc_ids, w_q, w_k, w_v, w_o):
        tokens = hidden.shape[0]
        seq = tokens * n_dev
        group = w_q.shape[1] // w_k.shape[1]
        freqs = rope_freqs()
        me = lax.axis_index("sp").astype(jnp.int32)
        me_arr = me[None]
        idx_all = lax.all_gather(jnp.stack([positions, doc_ids])[None], "sp", axis=0, tiled=True)
        idx_all, hidden, grad_out = lax.optimization_barrier((idx_all, hidden, grad_out))
        pos_all = idx_all[:, 0, :].reshape(seq)
        doc_all = idx_all[:, 1, :].reshape(seq)
        starts = jnp.sum((doc_all[None, :] < doc_all[:, None]).astype(jnp.int32), axis=1)
        first_blk = starts[::BLK] // BLK

        angles = positions.astype(F32)[:, None] * freqs[None, :]
        cos_loc, sin_loc = jnp.cos(angles), jnp.sin(angles)
        cos_tab = jnp.concatenate([cos_loc, cos_loc], axis=1)
        sin_tab = jnp.concatenate([-sin_loc, sin_loc], axis=1)
        angles_t = freqs[:, None] * pos_all.astype(F32)[None, :]
        cos_t, sin_t = jnp.cos(angles_t), jnp.sin(angles_t)

        every = tuple(range(n_dev))
        groups = ((0, 1), (2, 3, 4, 5), (6, 7))

        feats = group * HEAD_DIM

        def pairs(got, rels):
            return [part[r] for r in rels for part in got]

        def places(rels, parts=(0, 1)):
            return tuple((0, r, part * (feats // 2)) for r in rels for part in parts)

        half = hidden.shape[1] // 2
        x_got = reach(hidden[:, :half], hidden[:, half:])
        packed = project(hidden, grad_out, w_q, w_k, w_v, w_o, cos_tab, sin_tab, n_dev, group)
        packed = lax.all_to_all(packed, "sp", 0, 0, tiled=True).reshape(seq, -1)
        relay(x_got)
        near, far = tuple(range(6)), (6, 7)
        x_turned = assemble(x_got, near, n_dev, None, me_arr, True)
        g_got = reach(grad_out[:, :half], grad_out[:, half:])
        ctx_lo, ctx_hi, dq_lo, dq_hi, dk_t, dv_t = attention(packed, first_blk, starts[None, :], cos_t, sin_t, group)
        finish(x_got, dk_t)
        kv_got = reach(dk_t, dv_t)
        ctx_got = reach(ctx_lo, ctx_hi)
        dq_got = reach(dq_lo, dq_hi)

        x_turned = assemble(x_got, far, n_dev, x_turned, after(me_arr, dk_t), True)
        hold(g_got, x_turned)
        relay(g_got)
        (g_q,) = weight_grad([x_turned], pairs(dq_got, (0,)) + [swap(dq_got[0][0], CORE), swap(dq_got[1][0], CORE)], places(groups[0]), feats, me_arr, None, False, 1, n_dev)
        finish(g_got, g_q)
        g_all = [part[r] for part in g_got for r in every]
        (g_o,) = weight_grad(g_all, pairs(ctx_got, (0,)) + [swap(ctx_got[0][0], CORE), swap(ctx_got[1][0], CORE)], places(groups[0]), feats, after(me_arr, g_q), None, True, 1, n_dev)
        for rel in (SIDE_X, SIDE_Y):
            ctx_got[0][rel] = after(ctx_got[0][rel], g_o)
            ctx_got[0][rel | CORE] = swap(ctx_got[0][rel], CORE)
        (g_o,) = weight_grad(g_all, [ctx_got[0][r] for r in groups[1]], places(groups[1], (0,)), feats, me_arr, (g_o,), True, 1, n_dev)
        for rel in (SIDE_X, SIDE_Y):
            ctx_got[1][rel] = after(ctx_got[1][rel], g_o)
        relay(ctx_got)
        (g_o,) = weight_grad(g_all, [ctx_got[1][r] for r in groups[1]], places(groups[1], (1,)), feats, me_arr, (g_o,), True, 1, n_dev)
        finish(ctx_got, g_o)
        (g_o,) = weight_grad(g_all, pairs(ctx_got, groups[2]), places(groups[2]), feats, me_arr, (g_o,), True, 1, n_dev)
        hold(kv_got, g_o)
        relay(kv_got)
        attn_out = own_product([[[part[r] for part in ctx_got] for r in every]], [w_o], after(me_arr, g_o), tokens, False)
        finish(kv_got, attn_out)
        kv_places = tuple((o, r, 0) for o in range(2) for r in every)
        g_k, g_v = weight_grad([x_turned], [kv_got[0][r] for r in every] + [kv_got[1][r] for r in every], kv_places, HEAD_DIM, after(me_arr, attn_out), None, False, 2, n_dev)
        hold(dq_got, g_k)
        relay(dq_got)
        (g_q,) = weight_grad([x_turned], pairs(dq_got, groups[1]), places(groups[1]), feats, after(me_arr, g_k), (g_q,), False, 1, n_dev)
        finish(dq_got, g_q)
        (g_q,) = weight_grad([x_turned], pairs(dq_got, groups[2]), places(groups[2]), feats, me_arr, (g_q,), False, 1, n_dev)
        sources = [[[part[r] for part in dq_got] for r in every], [[kv_got[0][r]] for r in every], [[kv_got[1][r]] for r in every]]
        grad_hidden = own_product(sources, [w_q, w_k, w_v], after(me_arr, g_q), tokens, True)
        return attn_out, grad_hidden, g_q, g_k, g_v, g_o

    tok_spec = P(("dp", "sp"), None)
    vec_spec = P(("dp", "sp"))
    rep_spec = P(None, None)
    part_spec = P("dp", None)
    return jax.shard_map(device_body, mesh=mesh, in_specs=(tok_spec, tok_spec, vec_spec, vec_spec, rep_spec, rep_spec, rep_spec, rep_spec), out_specs=(tok_spec, tok_spec, part_spec, part_spec, part_spec, part_spec), check_vma=False)
```
